16 devices in a mesh: rep: 4 (over z, y), ep: 4 (over x, core).
Axes of the slice: x: 2, y: 2, z: 2, core: 2. Of those that a mesh axis runs over, the one named last changes fastest.
Arguments:
- x: bfloat16 [1024, 2048], P(('rep', 'ep')), parts along dimension 0
- cache: bfloat16 [1024, 256, 576], P(('rep', 'ep')), parts along dimension 0
- lens: int32 [1024], P(('rep', 'ep')), parts along dimension 0
- ids: int32 [1024, 6], P(('rep', 'ep')), parts along dimension 0
- rw: float32 [1024, 6], P(('rep', 'ep')), parts along dimension 0
- w_q: bfloat16 [2048, 3072], replicated
- w_dkv: bfloat16 [2048, 576], replicated
- w_uk: bfloat16 [16, 128, 512], replicated
- w_uv: bfloat16 [16, 512, 128], replicated
- w_o: bfloat16 [2048, 2048], replicated
- s_gate: bfloat16 [2048, 2816], replicated
- s_up: bfloat16 [2048, 2816], replicated
- s_down: bfloat16 [2816, 2048], replicated
- e_gate: bfloat16 [64, 2048, 1408], P('ep')
- e_up: bfloat16 [64, 2048, 1408], P('ep')
- e_down: bfloat16 [64, 1408, 2048], P('ep')
Outputs:
- output 1: bfloat16 [1024, 2048], P(('rep', 'ep')), parts along dimension 0
- output 2: bfloat16 [1024, 576], P(('rep', 'ep')), parts along dimension 0
There are 4 independent parts. The reference program is written for one: setup_inputs(seed, part) draws one part's arguments, and reference() takes and returns one part's arrays. A program takes and returns all parts, laid end to end along the dimension named above; an argument that names none is the same for every part.
All inputs are finite; a program needn't handle non-finite values.
Results may differ from the reference program's by a relative error of at most 0.0119234.
Values are sent between devices in bfloat16 or wider.
A program may use at most 1.5 GiB of HBM per device.

```python
import jax
import jax.numpy as jnp
from jax import lax

EP = 4
B_DEV = 64
L_MAX = 256
H = 2048
HEADS = 16
KV_LORA = 512
ROPE = 64
NOPE = 128
VHEAD = 128
EXPERTS = 64
TOP = 6
INTER = 1408
SHARED = 2816

B = EP * B_DEV
KVD = KV_LORA + ROPE
QKD = NOPE + ROPE
LEN_LO = (3 * L_MAX) // 4
EPS = 1e-6
ROPE_BASE = 1.0e4


def rms(v):
    v = v.astype(jnp.float32)
    return v * lax.rsqrt(jnp.mean(v * v, axis=-1, keepdims=True) + EPS)


def rope(v, pos):
    half = v.shape[-1] // 2
    inv = ROPE_BASE ** (-2.0 * jnp.arange(half, dtype=jnp.float32) / v.shape[-1])
    ang = pos.astype(jnp.float32)[..., None] * inv
    cs = jnp.cos(ang)
    sn = jnp.sin(ang)
    v1 = v[..., :half]
    v2 = v[..., half:]
    return jnp.concatenate([v1 * cs - v2 * sn, v2 * cs + v1 * sn], axis=-1)


def swiglu(u, wg, wu, wd):
    g = jnp.dot(u, wg, preferred_element_type=jnp.float32)
    v = jnp.dot(u, wu, preferred_element_type=jnp.float32)
    return jnp.dot((jax.nn.silu(g) * v).astype(jnp.bfloat16), wd, preferred_element_type=jnp.float32)


def setup_inputs(seed: int = 0, part: int = 0) -> dict:
    kbase = jax.random.fold_in(jax.random.key(seed), part)
    kp = jax.random.split(kbase, 8)
    kd = jax.random.split(jax.random.fold_in(kbase, 7), 3)
    kw = jax.random.split(jax.random.key(seed + 1), 11)

    def draw(k, shape, fan):
        return (jax.random.normal(k, shape, jnp.float32) * fan ** -0.5).astype(jnp.bfloat16)

    x = jax.random.normal(kp[0], (B, H), jnp.float32).astype(jnp.bfloat16)
    span = (L_MAX - LEN_LO) // 8
    dev = jnp.arange(B) // B_DEV
    low = jax.random.randint(kd[0], (B,), LEN_LO, LEN_LO + span)
    high = jax.random.randint(kd[1], (B,), L_MAX - span, L_MAX)
    lens = jnp.where(dev % 2 == 0, low, high).astype(jnp.int32)
    pos = jnp.arange(L_MAX)[None, :, None]
    m_live = 0.7 * jax.random.normal(kp[2], (B, 1, KVD), jnp.float32)
    m_old = 0.7 * jax.random.normal(kp[3], (B, 1, KVD), jnp.float32)
    noise = jax.random.normal(kp[4], (B, L_MAX, KVD), jnp.float32)
    cache = (jnp.where(pos < lens[:, None, None], m_live, m_old) + noise).astype(jnp.bfloat16)

    def route(k):
        k1, k2 = jax.random.split(k)
        perm_e = jax.random.permutation(k1, EXPERTS)
        perm_t = jax.random.permutation(k2, B_DEV)
        j = jnp.arange(B_DEV)[:, None] * TOP + jnp.arange(TOP)[None, :]
        return perm_e[j % (EXPERTS // 2)][perm_t]

    ids = jax.vmap(route)(jax.random.split(kd[2], EP)).reshape(B, TOP).astype(jnp.int32)
    rw = jax.random.uniform(kp[6], (B, TOP), jnp.float32, 0.5, 1.5) * TOP ** -0.5
    return {
        'x': x,
        'cache': cache,
        'lens': lens,
        'ids': ids,
        'rw': rw,
        'w_q': draw(kw[0], (H, HEADS * QKD), H),
        'w_dkv': draw(kw[1], (H, KVD), H),
        'w_uk': draw(kw[2], (HEADS, NOPE, KV_LORA), NOPE),
        'w_uv': draw(kw[3], (HEADS, KV_LORA, VHEAD), KV_LORA),
        'w_o': draw(kw[4], (HEADS * VHEAD, H), HEADS * VHEAD),
        's_gate': draw(kw[5], (H, SHARED), H),
        's_up': draw(kw[6], (H, SHARED), H),
        's_down': draw(kw[7], (SHARED, H), SHARED),
        'e_gate': draw(kw[8], (EXPERTS, H, INTER), H),
        'e_up': draw(kw[9], (EXPERTS, H, INTER), H),
        'e_down': draw(kw[10], (EXPERTS, INTER, H), INTER),
    }


def reference(x, cache, lens, ids, rw, w_q, w_dkv, w_uk, w_uv, w_o, s_gate, s_up, s_down, e_gate, e_up, e_down):
    xn = rms(x).astype(jnp.bfloat16)
    q = jnp.dot(xn, w_q, preferred_element_type=jnp.float32).astype(jnp.bfloat16).reshape(B, HEADS, QKD)
    kv = jnp.dot(xn, w_dkv, preferred_element_type=jnp.float32)
    kv_new = jnp.concatenate([rms(kv[:, :KV_LORA]), rope(kv[:, KV_LORA:], lens)], axis=-1).astype(jnp.bfloat16)
    q_lat = jnp.einsum('bhd,hdc->bhc', q[:, :, :NOPE].astype(jnp.float32), w_uk.astype(jnp.float32)).astype(jnp.bfloat16)
    q_rot = rope(q[:, :, NOPE:].astype(jnp.float32), lens[:, None]).astype(jnp.bfloat16)
    qf = jnp.concatenate([q_lat, q_rot], axis=-1)
    scale = QKD ** -0.5

    def attend(args):
        qb, cb, kb, lb = args
        qs = qb.astype(jnp.float32)
        cs = cb.astype(jnp.float32)
        ks = kb.astype(jnp.float32)
        s = jnp.dot(qs, cs.T) * scale
        s = jnp.where(jnp.arange(L_MAX)[None, :] < lb, s, -jnp.inf)
        s_new = jnp.dot(qs, ks) * scale
        mx = jnp.maximum(jnp.max(s, axis=1), s_new)
        e = jnp.exp(s - mx[:, None])
        e_new = jnp.exp(s_new - mx)
        den = jnp.sum(e, axis=1) + e_new
        p = (e / den[:, None]).astype(jnp.bfloat16).astype(jnp.float32)
        p_new = (e_new / den).astype(jnp.bfloat16).astype(jnp.float32)
        o = jnp.dot(p, cs[:, :KV_LORA]) + p_new[:, None] * ks[None, :KV_LORA]
        return o.astype(jnp.bfloat16)

    o_lat = lax.map(attend, (qf, cache, kv_new, lens))
    o = jnp.einsum('bhc,hcv->bhv', o_lat.astype(jnp.float32), w_uv.astype(jnp.float32)).astype(jnp.bfloat16).reshape(B, HEADS * VHEAD)
    a = jnp.dot(o, w_o, preferred_element_type=jnp.float32)
    h1 = (x.astype(jnp.float32) + a).astype(jnp.bfloat16)
    u = rms(h1).astype(jnp.bfloat16)
    shared = swiglu(u, s_gate, s_up, s_down)
    gate_w = jnp.sum(jnp.where(ids[:, :, None] == jnp.arange(EXPERTS)[None, None, :], rw[:, :, None], 0.0), axis=1)

    def expert(acc, args):
        wg, wu, wd, cw = args
        out = swiglu(u, wg, wu, wd).astype(jnp.bfloat16).astype(jnp.float32)
        return acc + cw[:, None] * out, None

    routed, _ = lax.scan(expert, jnp.zeros((B, H), jnp.float32), (e_gate, e_up, e_down, gate_w.T))
    y = (h1.astype(jnp.float32) + shared + routed).astype(jnp.bfloat16)
    return y, kv_new
```

```python
import math

import numpy as np
import jax
import jax.numpy as jnp
from jax import lax
from jax.experimental import pallas as pl
from jax.experimental.pallas import tpu as pltpu
from jax.sharding import PartitionSpec as P

EPS = 1e-6
ROPE_BASE = 1.0e4
CAP_FACTOR = 2
F32 = jnp.float32
BF16 = jnp.bfloat16
NSLOT = 5
NCACHE = 6
GROUP = 8
NCHUNK = 4
MESH = pl.DeviceIdType.MESH


def dot(a, b):
    return jnp.dot(a, b, preferred_element_type=F32)


def dot_nt(a, b):
    return lax.dot_general(a, b, (((1,), (1,)), ((), ())), preferred_element_type=F32)


def rms(v):
    return v * lax.rsqrt(jnp.mean(v * v, axis=-1, keepdims=True) + EPS)


def silu(g):
    return g / (1.0 + jnp.exp(-g))


def tiles(width, step):
    return [(a, min(step, width - a)) for a in range(0, width, step)]


def iota(shape, dim):
    return lax.broadcasted_iota(jnp.int32, shape, dim)


def layer_kernel(cape, lens_s, lens_v, inv, x, ids, rw, cache, w_q, w_dkv, w_uk, w_uv, w_o, s_gate, s_up, s_down, e_gate, e_up, e_down,
                 y, kvn,
                 ring, cbuf, dkv_b, uk_b, uv_b, q_s, qf, kv_s, o_s, h1_s, u_all, gw_all, d_s, w_s, xr, acts, acts_sh, outs, rp, xs, rc, sh,
                 ring_sem, c_sem, w_sem, gw_send, gw_recv, u_send, u_recv, p_send, p_recv, x_send, x_recv):
    bsz, hid = x.shape
    heads, nope, kvl = w_uk.shape
    kvd = cache.shape[2]
    lmax = cache.shape[1]
    qkd = nope + kvd - kvl
    vh = w_uv.shape[2]
    n_loc = e_gate.shape[0]
    inter = e_gate.shape[2]
    n_dev = gw_all.shape[0] // bsz
    rows_e = n_dev * cape
    cw = hid // NCHUNK
    grows = GROUP * heads
    nlat = kvl // 128
    cb = cw // 128
    me = lax.axis_index("ep")

    def peer(k):
        return jnp.bitwise_xor(me, k)

    barrier = pltpu.get_barrier_semaphore()
    for k in range(1, n_dev):
        pl.semaphore_signal(barrier, inc=1, device_id={"ep": peer(k)}, device_id_type=MESH)

    def to_slot(src, slot, rows=None, cols=None):
        dst = ring.at[slot]
        if rows is not None:
            dst = ring.at[slot, pl.ds(0, rows), pl.ds(0, cols)]
        return pltpu.make_async_copy(src, dst, ring_sem.at[slot])

    def wq_job(i):
        a = i * inter
        w = min(inter, w_q.shape[1] - a)
        return to_slot(w_q.at[:, pl.ds(a, w)], i, hid, w)

    def wo_job(i):
        a = i * inter
        w = min(inter, hid - a)
        return to_slot(w_o.at[:, pl.ds(a, w)], 3 + i, heads * vh, w)

    def sgu_job(i):
        src = s_gate if i % 2 == 0 else s_up
        return to_slot(src.at[:, pl.ds((i // 2) * inter, inter)], (5 + i) % NSLOT)

    def gate_job(e):
        return to_slot(e_gate.at[e], lax.rem(9 + 2 * e, NSLOT))

    def up_job(e):
        return to_slot(e_up.at[e], lax.rem(10 + 2 * e, NSLOT))

    def down_job(i):
        e = lax.rem(i, n_loc)
        c = pl.multiple_of((i // n_loc) * cw, cw)
        return to_slot(e_down.at[e, :, pl.ds(c, cw)], lax.rem(41 + i, NSLOT), inter, cw)

    def sd_job(i):
        r = i % 2
        c = i // 2
        half = hid // 2
        return to_slot(s_down.at[pl.ds(r * inter, inter), pl.ds(c * half, half)], (105 + i) % NSLOT, inter, half)

    def cache_job(g):
        s = lax.rem(g, NCACHE)
        return pltpu.make_async_copy(cache.at[pl.ds(g * GROUP, GROUP)], cbuf.at[s], c_sem.at[s])

    dkv_copy = pltpu.make_async_copy(w_dkv, dkv_b, w_sem.at[0])
    uk_copy = pltpu.make_async_copy(w_uk, uk_b, w_sem.at[1])
    uv_copy = pltpu.make_async_copy(w_uv, uv_b, w_sem.at[2])
    for i in range(3):
        wq_job(i).start()
    dkv_copy.start()
    uk_copy.start()
    for g in range(NCACHE):
        cache_job(g).start()
    uv_copy.start()
    for i in range(2):
        wo_job(i).start()

    col = iota((bsz, 128), 1)
    gw = jnp.zeros((bsz, 128), F32)
    for k in range(ids.shape[1]):
        gw = gw + jnp.where(ids[:, k:k + 1] == col, rw[:, k:k + 1], 0.0)
    gw_all[pl.ds(pl.multiple_of(me * bsz, bsz), bsz), :] = gw

    diag = iota((bsz, bsz), 0) == iota((bsz, bsz), 1)
    pos = jnp.sum(jnp.where(diag, jnp.broadcast_to(lens_v[...], (bsz, bsz)), 0), axis=1, keepdims=True).astype(F32)
    ang = pos * inv[...]
    cs = jnp.cos(ang)
    half = (kvd - kvl) // 2
    low = col < half
    sn = jnp.where(low, -1.0, 1.0) * jnp.sin(ang)

    def rope(v):
        sw = jnp.where(low, pltpu.roll(v, 128 - half, 1), pltpu.roll(v, half, 1))
        return v * cs + sw * sn

    xf = x[...].astype(F32)
    xn = rms(xf).astype(BF16)

    pl.semaphore_wait(barrier, n_dev - 1)

    def gw_copy(k):
        mine = gw_all.at[pl.ds(pl.multiple_of(me * bsz, bsz), bsz)]
        return pltpu.make_async_remote_copy(mine, mine, gw_send.at[k - 1], gw_recv.at[k - 1], device_id={"ep": peer(k)}, device_id_type=MESH)

    for k in range(1, n_dev):
        gw_copy(k).start()

    for i in range(3):
        wq_job(i).wait()
        a = i * inter
        for b, w in tiles(min(inter, w_q.shape[1] - a), 512):
            q_s[:, a + b:a + b + w] = dot(xn, ring[i, :, b:b + w]).astype(BF16)
    dkv_copy.wait()
    kv = dot(xn, dkv_b[...])
    kv_s[...] = jnp.zeros_like(kv_s)
    kv_s[:, :kvd] = kv
    kvn[:, :kvl] = rms(kv_s[:, :kvl]).astype(BF16)
    kvn[:, kvl:] = rope(kv_s[:, kvl:kvl + 128])[:, :kvd - kvl].astype(BF16)

    uk_copy.wait()
    left = col < 64

    def put_head(h, q_nope, q_rot):
        ql = dot(q_nope.astype(BF16), uk_b[h])
        for c in range(nlat):
            qf[c, pl.ds(h, bsz, stride=heads), :] = ql[:, 128 * c:128 * (c + 1)]
        qf[nlat, pl.ds(h, bsz, stride=heads), :] = jnp.where(left, rope(q_rot), 0.0)

    for hp in range(heads // 2):
        a = hp * 2 * qkd
        b0 = q_s[:, a:a + 128].astype(F32)
        b1 = q_s[:, a + 128:a + 256].astype(F32)
        b2 = q_s[:, a + 256:a + 384].astype(F32)
        r1 = pltpu.roll(b1, 64, 1)
        r2 = pltpu.roll(b2, 64, 1)
        put_head(2 * hp, b0, b1)
        put_head(2 * hp + 1, jnp.where(left, r1, r2), r2)

    scale = qkd ** -0.5
    tpos = iota((heads, lmax), 1)
    seq_of_row = iota((grows, bsz), 0) // heads
    seq_col = iota((grows, bsz), 1)

    def attend(g, carry):
        s = lax.rem(g, NCACHE)
        cache_job(g).wait()
        rows = pl.ds(pl.multiple_of(g * grows, grows), grows)
        qg = jnp.concatenate([qf[c, rows, :].astype(BF16) for c in range(nlat + 1)], axis=1)[:, :kvd]
        own = seq_col == seq_of_row + g * GROUP
        s_new = jnp.sum(jnp.where(own, dot_nt(qg, kvn[...]), 0.0), axis=1, keepdims=True) * scale
        parts = []
        for i in range(GROUP):
            si = dot_nt(qg[i * heads:(i + 1) * heads], cbuf[s, i]) * scale
            parts.append(jnp.where(tpos < lens_s[g * GROUP + i], si, -jnp.inf))
        sc = jnp.concatenate(parts, axis=0)
        mx = jnp.maximum(jnp.max(sc, axis=1, keepdims=True), s_new)
        e = jnp.exp(sc - mx)
        e_new = jnp.exp(s_new - mx)
        den = jnp.sum(e, axis=1, keepdims=True) + e_new
        rden = 1.0 / den
        p = (e * rden).astype(BF16)
        p_new = jnp.where(own, e_new * rden, 0.0).astype(BF16)
        o_new = dot(p_new, kvn[:, :kvl])
        outs_i = [dot(p[i * heads:(i + 1) * heads], cbuf[s, i, :, :kvl]) for i in range(GROUP)]
        o_lat = jnp.concatenate(outs_i, axis=0) + o_new
        for c in range(nlat):
            qf[c, rows, :] = o_lat[:, 128 * c:128 * (c + 1)]

        @pl.when(g + NCACHE < bsz // GROUP)
        def _():
            cache_job(g + NCACHE).start()

        @pl.when(g == bsz // GROUP - NCACHE - 1)
        def _():
            for i in range(3):
                sgu_job(i).start()
        return carry

    lax.fori_loop(0, bsz // GROUP, attend, 0)

    uv_copy.wait()
    for h in range(heads):
        oh = jnp.concatenate([qf[c, pl.ds(h, bsz, stride=heads), :].astype(BF16) for c in range(nlat)], axis=1)
        o_s[:, h * vh:(h + 1) * vh] = dot(oh, uv_b[h]).astype(BF16)
    for i in range(2):
        wo_job(i).wait()
        a = i * inter
        for b, w in tiles(min(inter, hid - a), 512):
            h1_s[:, a + b:a + b + w] = (x[:, a + b:a + b + w].astype(F32) + dot(o_s[...], ring[3 + i, :, b:b + w])).astype(BF16)
    sgu_job(3).start()
    gate_job(0).start()

    u = rms(h1_s[...].astype(F32)).astype(BF16)
    mine = pl.ds(pl.multiple_of(me * bsz, bsz), bsz)
    across = pl.ds(pl.multiple_of(peer(2) * bsz, bsz), bsz)
    u_all[mine, :] = u

    def u_copy(rows, i, k):
        blk = u_all.at[rows]
        return pltpu.make_async_remote_copy(blk, blk, u_send.at[i], u_recv.at[i], device_id={"ep": peer(k)}, device_id_type=MESH)

    u_copy(mine, 1, 2).start()
    u_copy(mine, 0, 1).start()

    def shared_gu(i):
        for j in range(2):
            sgu_job(2 * i + j).wait()
        uu = u_all[mine, :]
        for b, w in tiles(inter, 512):
            gg = dot(uu, ring[(5 + 2 * i) % NSLOT, :, b:b + w])
            vv = dot(uu, ring[(6 + 2 * i) % NSLOT, :, b:b + w])
            acts_sh[:, i * inter + b:i * inter + b + w] = (silu(gg) * vv).astype(BF16)

    shared_gu(0)
    up_job(0).start()
    gate_job(1).start()
    shared_gu(1)
    up_job(1).start()
    gate_job(2).start()

    for k in range(1, n_dev):
        gw_copy(k).wait()
    nt = n_dev * bsz
    ga = gw_all[...]
    hit = ga > 0.0
    ti = iota((nt, nt), 0)
    tj = iota((nt, nt), 1)
    before = ((ti // bsz == tj // bsz) & (tj < ti)).astype(F32).astype(BF16)
    rank = dot(before, jnp.where(hit, 1.0, 0.0).astype(BF16))
    src = (iota((nt, 128), 0) // bsz * cape).astype(F32)
    code = jnp.where(hit, src + rank, -1.0)
    exp_r = iota((128, n_loc * rows_e), 0)
    exp_c = iota((128, n_loc * rows_e), 1) // rows_e
    spread = (exp_r == exp_c + me * n_loc).astype(F32).astype(BF16)
    code_x = dot(code.astype(BF16), spread)
    slot_c = (iota((nt, n_loc * rows_e), 1) % rows_e).astype(F32)
    member = code_x == slot_c
    g1 = ga.astype(BF16)
    res = ga - g1.astype(F32)
    g2 = res.astype(BF16)
    g3 = (res - g2.astype(F32)).astype(BF16)
    for t, gt in enumerate((g1, g2, g3)):
        w_s[t] = jnp.where(member, dot(gt, spread), 0.0).astype(BF16)
    d_s[...] = jnp.where(member, 1.0, 0.0).T.astype(BF16)

    u_copy(mine, 1, 2).wait_recv()
    u_copy(across, 2, 1).start()
    u_copy(mine, 0, 1).wait()
    u_copy(across, 2, 1).wait()
    u_copy(mine, 1, 2).wait_send()

    def gate_up(e, carry):
        erows = pl.ds(pl.multiple_of(e * rows_e, rows_e), rows_e)
        de = d_s[erows, :]
        for b, w in tiles(hid, 512):
            xr[:, b:b + w] = dot(de, u_all[:, b:b + w]).astype(BF16)
        gate_job(e).wait()
        up_job(e).wait()
        sg = lax.rem(9 + 2 * e, NSLOT)
        su = lax.rem(10 + 2 * e, NSLOT)
        for b, w in tiles(inter, 512):
            gg = dot(xr[...], ring[sg, :, b:b + w])
            vv = dot(xr[...], ring[su, :, b:b + w])
            acts[erows, b:b + w] = (silu(gg) * vv).astype(BF16)

        @pl.when(e + 2 < n_loc)
        def _():
            up_job(e + 2).start()

        @pl.when(e + 2 >= n_loc)
        def _():
            down_job(14 + 2 * e - 41).start()

        @pl.when(e + 3 < n_loc)
        def _():
            gate_job(e + 3).start()

        @pl.when(e + 3 >= n_loc)
        def _():
            down_job(15 + 2 * e - 41).start()
        return carry

    lax.fori_loop(0, n_loc, gate_up, 0)

    def part(j, d):
        return pl.ds(pl.multiple_of(j * nt + d * bsz, bsz), bsz)

    def pair_copy(j, i, d):
        return pltpu.make_async_remote_copy(qf.at[pl.ds(0, cb), part(j, d)], rp.at[i, pl.ds(j * cb, cb)],
                                            p_send.at[j, i], p_recv.at[j, i], device_id={"ep": peer(1)}, device_id_type=MESH)

    def cross_copy(j):
        blk = pl.ds(j * cb, cb)
        return pltpu.make_async_remote_copy(xs.at[blk], rc.at[blk], x_send.at[j], x_recv.at[j],
                                            device_id={"ep": peer(2)}, device_id_type=MESH)

    def start_pair(j):
        pair_copy(j, 1, peer(3)).start()
        pair_copy(j, 0, peer(1)).start()

    def forward(j):
        pair_copy(j, 1, peer(3)).wait_recv()
        for c in range(cb):
            xs[j * cb + c] = qf[c, part(j, peer(2)), :] + rp[1, j * cb + c]
        cross_copy(j).start()

    for j in range(NCHUNK):
        def down(e, carry):
            i = j * n_loc + e
            down_job(i).wait()
            erows = pl.ds(pl.multiple_of(e * rows_e, rows_e), rows_e)
            outs[erows, :] = dot(acts[erows, :], ring[lax.rem(41 + i, NSLOT), :inter, :cw]).astype(BF16)
            if j < NCHUNK - 1:
                down_job(i + NSLOT).start()
            else:
                @pl.when(e + NSLOT < n_loc)
                def _():
                    down_job(i + NSLOT).start()
                for k in range(4):
                    @pl.when(e == n_loc - NSLOT + k)
                    def _():
                        sd_job(k).start()
            return carry

        lax.fori_loop(0, n_loc, down, 0)
        if j >= 1:
            forward(j - 1)
        ov = outs[...]
        total = dot(w_s[0], ov) + dot(w_s[1], ov) + dot(w_s[2], ov)
        for c in range(cb):
            qf[c, pl.ds(j * nt, nt), :] = total[:, 128 * c:128 * (c + 1)]
        start_pair(j)

    hw = hid // 2
    for c in range(2):
        for r in range(2):
            sd_job(2 * c + r).wait()
        for b, w in tiles(hw, 512):
            acc = dot(acts_sh[:, :inter], ring[(105 + 2 * c) % NSLOT, :inter, b:b + w])
            acc += dot(acts_sh[:, inter:], ring[(106 + 2 * c) % NSLOT, :inter, b:b + w])
            sh[:, c * hw + b:c * hw + b + w] = acc
        if c == 0:
            forward(NCHUNK - 1)

    for j in range(NCHUNK):
        pair_copy(j, 0, peer(1)).wait_recv()
        cross_copy(j).wait_recv()
        for c in range(cb):
            b = j * cb + c
            cols = slice(b * 128, (b + 1) * 128)
            routed = qf[c, part(j, me), :] + rp[0, b] + rc[b]
            y[:, cols] = (h1_s[:, cols].astype(F32) + sh[:, cols] + routed).astype(BF16)
    for j in range(NCHUNK):
        pair_copy(j, 1, peer(3)).wait_send()
        pair_copy(j, 0, peer(1)).wait_send()
        cross_copy(j).wait_send()


def solution(mesh):
    n = mesh.shape['ep']
    tok_spec = P(('rep', 'ep'))
    row_spec = P(('rep', 'ep'), None)
    cache_spec = P(('rep', 'ep'), None, None)
    exp_spec = P('ep', None, None)

    def local(x, cache, lens, ids, rw, w_q, w_dkv, w_uk, w_uv, w_o, s_gate, s_up, s_down, e_gate, e_up, e_down):
        bsz, hid = x.shape
        heads, nope, kvl = w_uk.shape
        lmax, kvd = cache.shape[1:]
        n_loc, _, inter = e_gate.shape
        top = ids.shape[1]
        n_exp = n_loc * n
        cape = (CAP_FACTOR * bsz * top + n_exp - 1) // n_exp
        rows_e = n * cape
        nt = n * bsz
        cw = hid // NCHUNK
        half = (kvd - kvl) // 2
        inv = np.float64(ROPE_BASE) ** (-2.0 * (np.arange(128) % half) / (kvd - kvl))
        inv = jnp.asarray(inv.astype(np.float32)[None, :])
        vm = pl.BlockSpec(memory_space=pltpu.VMEM)
        hb = pl.BlockSpec(memory_space=pl.ANY)
        dma = pltpu.SemaphoreType.DMA
        call = pl.pallas_call(
            lambda *refs: layer_kernel(cape, *refs),
            name="layer",
            out_shape=(jax.ShapeDtypeStruct((bsz, hid), BF16), jax.ShapeDtypeStruct((bsz, kvd), BF16)),
            in_specs=[pl.BlockSpec(memory_space=pltpu.SMEM)] + [vm] * 5 + [hb] * 12,
            out_specs=(vm, vm),
            scratch_shapes=[
                pltpu.VMEM((NSLOT, hid, inter), BF16),
                pltpu.VMEM((NCACHE, GROUP, lmax, kvd), BF16),
                pltpu.VMEM(w_dkv.shape, BF16),
                pltpu.VMEM(w_uk.shape, BF16),
                pltpu.VMEM(w_uv.shape, BF16),
                pltpu.VMEM((bsz, w_q.shape[1]), BF16),
                pltpu.VMEM((kvl // 128 + 1, bsz * heads, 128), F32),
                pltpu.VMEM((bsz, kvl + 128), F32),
                pltpu.VMEM((bsz, hid), BF16),
                pltpu.VMEM((bsz, hid), BF16),
                pltpu.VMEM((nt, hid), BF16),
                pltpu.VMEM((nt, 128), F32),
                pltpu.VMEM((n_loc * rows_e, nt), BF16),
                pltpu.VMEM((3, nt, n_loc * rows_e), BF16),
                pltpu.VMEM((rows_e, hid), BF16),
                pltpu.VMEM((n_loc * rows_e, inter), BF16),
                pltpu.VMEM((bsz, 2 * inter), BF16),
                pltpu.VMEM((n_loc * rows_e, cw), BF16),
                pltpu.VMEM((2, hid // 128, bsz, 128), F32),
                pltpu.VMEM((hid // 128, bsz, 128), F32),
                pltpu.VMEM((hid // 128, bsz, 128), F32),
                pltpu.VMEM((bsz, hid), F32),
                dma((NSLOT,)), dma((NCACHE,)), dma((3,)),
                dma((n - 1,)), dma((n - 1,)), dma((3,)), dma((3,)),
                dma((NCHUNK, 2)), dma((NCHUNK, 2)), dma((NCHUNK,)), dma((NCHUNK,)),
            ],
            compiler_params=pltpu.CompilerParams(collective_id=0, has_side_effects=True, vmem_limit_bytes=67_043_328),
        )
        return call(lens, lens.reshape(1, bsz), inv, x, ids, rw, cache, w_q, w_dkv, w_uk, w_uv, w_o, s_gate, s_up, s_down, e_gate, e_up, e_down)

    in_specs = (row_spec, cache_spec, tok_spec, row_spec, row_spec) + (P(),) * 8 + (exp_spec,) * 3
    return jax.shard_map(local, mesh=mesh, in_specs=in_specs, out_specs=(row_spec, row_spec), check_vma=False)
```

```python
import math

import numpy as np
import jax
import jax.numpy as jnp
from jax import lax
from jax.experimental import pallas as pl
from jax.experimental.pallas import tpu as pltpu
from jax.sharding import PartitionSpec as P

EPS = 1e-6
ROPE_BASE = 1.0e4
CAP_FACTOR = 2
F32 = jnp.float32
BF16 = jnp.bfloat16
NSLOT = 5
NCACHE = 6
GROUP = 8
NCHUNK = 4
MESH = pl.DeviceIdType.MESH


def dot(a, b):
    return jnp.dot(a, b, preferred_element_type=F32)


def dot_nt(a, b):
    return lax.dot_general(a, b, (((1,), (1,)), ((), ())), preferred_element_type=F32)


def rms(v):
    return v * lax.rsqrt(jnp.mean(v * v, axis=-1, keepdims=True) + EPS)


def silu(g):
    return g / (1.0 + jnp.exp(-g))


def tiles(width, step):
    return [(a, min(step, width - a)) for a in range(0, width, step)]


def iota(shape, dim):
    return lax.broadcasted_iota(jnp.int32, shape, dim)


def layer_kernel(cape, lens_s, lens_v, inv, x, ids, rw, cache, w_q, w_dkv, w_uk, w_uv, w_o, s_gate, s_up, s_down, e_gate, e_up, e_down,
                 y, kvn,
                 ring, cbuf, dkv_b, uk_b, uv_b, q_s, qf, kv_s, o_s, h1_s, u_all, gw_all, d_s, w_s, xr, acts, acts_sh, outs, rp, xs, rc, sh,
                 ring_sem, c_sem, w_sem, gw_send, gw_recv, u_send, u_recv, p_send, p_recv, x_send, x_recv):
    bsz, hid = x.shape
    heads, nope, kvl = w_uk.shape
    kvd, lmax = cache.shape[1:]
    qkd = nope + kvd - kvl
    vh = w_uv.shape[2]
    n_loc = e_gate.shape[0]
    inter = e_gate.shape[2]
    n_dev = gw_all.shape[0] // bsz
    rows_e = n_dev * cape
    cw = hid // NCHUNK
    grows = GROUP * heads
    nlat = kvl // 128
    cb = cw // 128
    me = lax.axis_index("ep")

    def peer(k):
        return jnp.bitwise_xor(me, k)

    barrier = pltpu.get_barrier_semaphore()
    for k in range(1, n_dev):
        pl.semaphore_signal(barrier, inc=1, device_id={"ep": peer(k)}, device_id_type=MESH)

    def to_slot(src, slot, rows=None, cols=None):
        dst = ring.at[slot]
        if rows is not None:
            dst = ring.at[slot, pl.ds(0, rows), pl.ds(0, cols)]
        return pltpu.make_async_copy(src, dst, ring_sem.at[slot])

    def wq_job(i):
        a = i * inter
        w = min(inter, w_q.shape[1] - a)
        return to_slot(w_q.at[:, pl.ds(a, w)], i, hid, w)

    def wo_job(i):
        a = i * inter
        w = min(inter, hid - a)
        return to_slot(w_o.at[:, pl.ds(a, w)], 3 + i, heads * vh, w)

    def sgu_job(i):
        src = s_gate if i % 2 == 0 else s_up
        return to_slot(src.at[:, pl.ds((i // 2) * inter, inter)], (5 + i) % NSLOT)

    def gate_job(e):
        return to_slot(e_gate.at[e], lax.rem(9 + 2 * e, NSLOT))

    def up_job(e):
        return to_slot(e_up.at[e], lax.rem(10 + 2 * e, NSLOT))

    def down_job(i):
        e = lax.rem(i, n_loc)
        c = pl.multiple_of((i // n_loc) * cw, cw)
        return to_slot(e_down.at[e, :, pl.ds(c, cw)], lax.rem(41 + i, NSLOT), inter, cw)

    def sd_job(i):
        r = i % 2
        c = i // 2
        half = hid // 2
        return to_slot(s_down.at[pl.ds(r * inter, inter), pl.ds(c * half, half)], (105 + i) % NSLOT, inter, half)

    def cache_job(g):
        s = lax.rem(g, NCACHE)
        return pltpu.make_async_copy(cache.at[pl.ds(g * GROUP, GROUP)], cbuf.at[s], c_sem.at[s])

    dkv_copy = pltpu.make_async_copy(w_dkv, dkv_b, w_sem.at[0])
    uk_copy = pltpu.make_async_copy(w_uk, uk_b, w_sem.at[1])
    uv_copy = pltpu.make_async_copy(w_uv, uv_b, w_sem.at[2])
    for i in range(3):
        wq_job(i).start()
    dkv_copy.start()
    uk_copy.start()
    for g in range(NCACHE):
        cache_job(g).start()
    uv_copy.start()
    for i in range(2):
        wo_job(i).start()

    col = iota((bsz, 128), 1)
    expert = iota((128, bsz), 0)
    gw = jnp.zeros((128, bsz), F32)
    for k in range(ids.shape[0]):
        gw = gw + jnp.where(ids[k:k + 1, :] == expert, rw[k:k + 1, :], 0.0)
    gw_all[pl.ds(pl.multiple_of(me * bsz, bsz), bsz), :] = gw.T

    diag = iota((bsz, bsz), 0) == iota((bsz, bsz), 1)
    pos = jnp.sum(jnp.where(diag, jnp.broadcast_to(lens_v[...], (bsz, bsz)), 0), axis=1, keepdims=True).astype(F32)
    ang = pos * inv[...]
    cs = jnp.cos(ang)
    half = (kvd - kvl) // 2
    low = col < half
    sn = jnp.where(low, -1.0, 1.0) * jnp.sin(ang)

    def rope(v):
        sw = jnp.where(low, pltpu.roll(v, 128 - half, 1), pltpu.roll(v, half, 1))
        return v * cs + sw * sn

    xf = x[...].astype(F32)
    xn = rms(xf).astype(BF16)

    pl.semaphore_wait(barrier, n_dev - 1)

    def gw_copy(k):
        mine = gw_all.at[pl.ds(pl.multiple_of(me * bsz, bsz), bsz)]
        return pltpu.make_async_remote_copy(mine, mine, gw_send.at[k - 1], gw_recv.at[k - 1], device_id={"ep": peer(k)}, device_id_type=MESH)

    for k in range(1, n_dev):
        gw_copy(k).start()

    for i in range(3):
        wq_job(i).wait()
        a = i * inter
        for b, w in tiles(min(inter, w_q.shape[1] - a), 512):
            q_s[:, a + b:a + b + w] = dot(xn, ring[i, :, b:b + w]).astype(BF16)
    dkv_copy.wait()
    kv = dot_nt(xn, dkv_b[...])
    kv_s[...] = jnp.zeros_like(kv_s)
    kv_s[:, :kvd] = kv
    kvn[:, :kvl] = rms(kv_s[:, :kvl]).astype(BF16)
    kvn[:, kvl:] = rope(kv_s[:, kvl:kvl + 128])[:, :kvd - kvl].astype(BF16)

    uk_copy.wait()
    left = col < 64

    def put_head(h, q_nope, q_rot):
        ql = dot(q_nope.astype(BF16), uk_b[h])
        for c in range(nlat):
            qf[c, pl.ds(h, bsz, stride=heads), :] = ql[:, 128 * c:128 * (c + 1)]
        qf[nlat, pl.ds(h, bsz, stride=heads), :] = jnp.where(left, rope(q_rot), 0.0)

    for hp in range(heads // 2):
        a = hp * 2 * qkd
        b0 = q_s[:, a:a + 128].astype(F32)
        b1 = q_s[:, a + 128:a + 256].astype(F32)
        b2 = q_s[:, a + 256:a + 384].astype(F32)
        r1 = pltpu.roll(b1, 64, 1)
        r2 = pltpu.roll(b2, 64, 1)
        put_head(2 * hp, b0, b1)
        put_head(2 * hp + 1, jnp.where(left, r1, r2), r2)

    scale = qkd ** -0.5
    tpos = iota((heads, lmax), 1)
    seq_of_row = iota((grows, bsz), 0) // heads
    seq_col = iota((grows, bsz), 1)

    def attend(g, carry):
        s = lax.rem(g, NCACHE)
        cache_job(g).wait()
        rows = pl.ds(pl.multiple_of(g * grows, grows), grows)
        qg = jnp.concatenate([qf[c, rows, :].astype(BF16) for c in range(nlat + 1)], axis=1)[:, :kvd]
        own = seq_col == seq_of_row + g * GROUP
        s_new = jnp.sum(jnp.where(own, dot_nt(qg, kvn[...]), 0.0), axis=1, keepdims=True) * scale
        parts = []
        for i in range(GROUP):
            si = dot(qg[i * heads:(i + 1) * heads], cbuf[s, i]) * scale
            parts.append(jnp.where(tpos < lens_s[g * GROUP + i], si, -jnp.inf))
        sc = jnp.concatenate(parts, axis=0)
        mx = jnp.maximum(jnp.max(sc, axis=1, keepdims=True), s_new)
        e = jnp.exp(sc - mx)
        e_new = jnp.exp(s_new - mx)
        den = jnp.sum(e, axis=1, keepdims=True) + e_new
        rden = 1.0 / den
        p = (e * rden).astype(BF16)
        p_new = jnp.where(own, e_new * rden, 0.0).astype(BF16)
        o_new = dot(p_new, kvn[:, :kvl])
        outs_i = [dot_nt(p[i * heads:(i + 1) * heads], cbuf[s, i, :kvl, :]) for i in range(GROUP)]
        o_lat = jnp.concatenate(outs_i, axis=0) + o_new
        for c in range(nlat):
            qf[c, rows, :] = o_lat[:, 128 * c:128 * (c + 1)]

        @pl.when(g + NCACHE < bsz // GROUP)
        def _():
            cache_job(g + NCACHE).start()

        @pl.when(g == bsz // GROUP - NCACHE - 1)
        def _():
            for i in range(3):
                sgu_job(i).start()
        return carry

    lax.fori_loop(0, bsz // GROUP, attend, 0)

    uv_copy.wait()
    for h in range(heads):
        oh = jnp.concatenate([qf[c, pl.ds(h, bsz, stride=heads), :].astype(BF16) for c in range(nlat)], axis=1)
        o_s[:, h * vh:(h + 1) * vh] = dot(oh, uv_b[h]).astype(BF16)
    for i in range(2):
        wo_job(i).wait()
        a = i * inter
        for b, w in tiles(min(inter, hid - a), 512):
            h1_s[:, a + b:a + b + w] = (x[:, a + b:a + b + w].astype(F32) + dot(o_s[...], ring[3 + i, :, b:b + w])).astype(BF16)
    sgu_job(3).start()
    gate_job(0).start()

    u = rms(h1_s[...].astype(F32)).astype(BF16)
    mine = pl.ds(pl.multiple_of(me * bsz, bsz), bsz)
    across = pl.ds(pl.multiple_of(peer(2) * bsz, bsz), bsz)
    u_all[mine, :] = u

    def u_copy(rows, i, k):
        blk = u_all.at[rows]
        return pltpu.make_async_remote_copy(blk, blk, u_send.at[i], u_recv.at[i], device_id={"ep": peer(k)}, device_id_type=MESH)

    u_copy(mine, 1, 2).start()
    u_copy(mine, 0, 1).start()

    def shared_gu(i):
        for j in range(2):
            sgu_job(2 * i + j).wait()
        uu = u_all[mine, :]
        for b, w in tiles(inter, 512):
            gg = dot(uu, ring[(5 + 2 * i) % NSLOT, :, b:b + w])
            vv = dot(uu, ring[(6 + 2 * i) % NSLOT, :, b:b + w])
            acts_sh[:, i * inter + b:i * inter + b + w] = (silu(gg) * vv).astype(BF16)

    shared_gu(0)
    up_job(0).start()
    gate_job(1).start()
    shared_gu(1)
    up_job(1).start()
    gate_job(2).start()

    for k in range(1, n_dev):
        gw_copy(k).wait()
    nt = n_dev * bsz
    ga = gw_all[...]
    hit = ga > 0.0
    ti = iota((nt, nt), 0)
    tj = iota((nt, nt), 1)
    before = ((ti // bsz == tj // bsz) & (tj < ti)).astype(F32).astype(BF16)
    rank = dot(before, jnp.where(hit, 1.0, 0.0).astype(BF16))
    src = (iota((nt, 128), 0) // bsz * cape).astype(F32)
    code = jnp.where(hit, src + rank, -1.0)
    exp_r = iota((128, n_loc * rows_e), 0)
    exp_c = iota((128, n_loc * rows_e), 1) // rows_e
    spread = (exp_r == exp_c + me * n_loc).astype(F32).astype(BF16)
    code_x = dot(code.astype(BF16), spread)
    slot_c = (iota((nt, n_loc * rows_e), 1) % rows_e).astype(F32)
    member = code_x == slot_c
    g1 = ga.astype(BF16)
    res = ga - g1.astype(F32)
    g2 = res.astype(BF16)
    g3 = (res - g2.astype(F32)).astype(BF16)
    for t, gt in enumerate((g1, g2, g3)):
        w_s[t] = jnp.where(member, dot(gt, spread), 0.0).astype(BF16)
    d_s[...] = jnp.where(member, 1.0, 0.0).T.astype(BF16)

    u_copy(mine, 1, 2).wait_recv()
    u_copy(across, 2, 1).start()
    u_copy(mine, 0, 1).wait()
    u_copy(across, 2, 1).wait()
    u_copy(mine, 1, 2).wait_send()

    def gate_up(e, carry):
        erows = pl.ds(pl.multiple_of(e * rows_e, rows_e), rows_e)
        de = d_s[erows, :]
        for b, w in tiles(hid, 512):
            xr[:, b:b + w] = dot(de, u_all[:, b:b + w]).astype(BF16)
        gate_job(e).wait()
        up_job(e).wait()
        sg = lax.rem(9 + 2 * e, NSLOT)
        su = lax.rem(10 + 2 * e, NSLOT)
        for b, w in tiles(inter, 512):
            gg = dot(xr[...], ring[sg, :, b:b + w])
            vv = dot(xr[...], ring[su, :, b:b + w])
            acts[erows, b:b + w] = (silu(gg) * vv).astype(BF16)

        @pl.when(e + 2 < n_loc)
        def _():
            up_job(e + 2).start()

        @pl.when(e + 2 >= n_loc)
        def _():
            down_job(14 + 2 * e - 41).start()

        @pl.when(e + 3 < n_loc)
        def _():
            gate_job(e + 3).start()

        @pl.when(e + 3 >= n_loc)
        def _():
            down_job(15 + 2 * e - 41).start()
        return carry

    lax.fori_loop(0, n_loc, gate_up, 0)

    def part(j, d):
        return pl.ds(pl.multiple_of(j * nt + d * bsz, bsz), bsz)

    def pair_copy(j, i, d):
        return pltpu.make_async_remote_copy(qf.at[pl.ds(0, cb), part(j, d)], rp.at[i, pl.ds(j * cb, cb)],
                                            p_send.at[j, i], p_recv.at[j, i], device_id={"ep": peer(1)}, device_id_type=MESH)

    def cross_copy(j):
        blk = pl.ds(j * cb, cb)
        return pltpu.make_async_remote_copy(xs.at[blk], rc.at[blk], x_send.at[j], x_recv.at[j],
                                            device_id={"ep": peer(2)}, device_id_type=MESH)

    def start_pair(j):
        pair_copy(j, 1, peer(3)).start()
        pair_copy(j, 0, peer(1)).start()

    def forward(j):
        pair_copy(j, 1, peer(3)).wait_recv()
        for c in range(cb):
            xs[j * cb + c] = qf[c, part(j, peer(2)), :] + rp[1, j * cb + c]
        cross_copy(j).start()

    for j in range(NCHUNK):
        def down(e, carry):
            i = j * n_loc + e
            down_job(i).wait()
            erows = pl.ds(pl.multiple_of(e * rows_e, rows_e), rows_e)
            outs[erows, :] = dot(acts[erows, :], ring[lax.rem(41 + i, NSLOT), :inter, :cw]).astype(BF16)
            if j < NCHUNK - 1:
                down_job(i + NSLOT).start()
            else:
                @pl.when(e + NSLOT < n_loc)
                def _():
                    down_job(i + NSLOT).start()
                for k in range(4):
                    @pl.when(e == n_loc - NSLOT + k)
                    def _():
                        sd_job(k).start()
            return carry

        lax.fori_loop(0, n_loc, down, 0)
        if j >= 1:
            forward(j - 1)
        ov = outs[...]
        total = dot(w_s[0], ov) + dot(w_s[1], ov) + dot(w_s[2], ov)
        for c in range(cb):
            qf[c, pl.ds(j * nt, nt), :] = total[:, 128 * c:128 * (c + 1)]
        start_pair(j)

    hw = hid // 2
    for c in range(2):
        for r in range(2):
            sd_job(2 * c + r).wait()
        for b, w in tiles(hw, 512):
            acc = dot(acts_sh[:, :inter], ring[(105 + 2 * c) % NSLOT, :inter, b:b + w])
            acc += dot(acts_sh[:, inter:], ring[(106 + 2 * c) % NSLOT, :inter, b:b + w])
            sh[:, c * hw + b:c * hw + b + w] = acc
        if c == 0:
            forward(NCHUNK - 1)

    for j in range(NCHUNK):
        pair_copy(j, 0, peer(1)).wait_recv()
        cross_copy(j).wait_recv()
        for c in range(cb):
            b = j * cb + c
            cols = slice(b * 128, (b + 1) * 128)
            routed = qf[c, part(j, me), :] + rp[0, b] + rc[b]
            y[:, cols] = (h1_s[:, cols].astype(F32) + sh[:, cols] + routed).astype(BF16)
    for j in range(NCHUNK):
        pair_copy(j, 1, peer(3)).wait_send()
        pair_copy(j, 0, peer(1)).wait_send()
        cross_copy(j).wait_send()


def solution(mesh):
    n = mesh.shape['ep']
    tok_spec = P(('rep', 'ep'))
    row_spec = P(('rep', 'ep'), None)
    cache_spec = P(('rep', 'ep'), None, None)
    exp_spec = P('ep', None, None)

    def local(x, cache, lens, ids, rw, w_q, w_dkv, w_uk, w_uv, w_o, s_gate, s_up, s_down, e_gate, e_up, e_down):
        bsz, hid = x.shape
        heads, nope, kvl = w_uk.shape
        lmax, kvd = cache.shape[1:]
        n_loc, _, inter = e_gate.shape
        top = ids.shape[1]
        n_exp = n_loc * n
        cape = (CAP_FACTOR * bsz * top + n_exp - 1) // n_exp
        rows_e = n * cape
        nt = n * bsz
        cw = hid // NCHUNK
        half = (kvd - kvl) // 2
        inv = np.float64(ROPE_BASE) ** (-2.0 * (np.arange(128) % half) / (kvd - kvl))
        inv = jnp.asarray(inv.astype(np.float32)[None, :])
        vm = pl.BlockSpec(memory_space=pltpu.VMEM)
        hb = pl.BlockSpec(memory_space=pl.ANY)
        dma = pltpu.SemaphoreType.DMA
        call = pl.pallas_call(
            lambda *refs: layer_kernel(cape, *refs),
            name="layer",
            out_shape=(jax.ShapeDtypeStruct((bsz, hid), BF16), jax.ShapeDtypeStruct((bsz, kvd), BF16)),
            in_specs=[pl.BlockSpec(memory_space=pltpu.SMEM)] + [vm] * 5 + [hb] * 12,
            out_specs=(vm, vm),
            scratch_shapes=[
                pltpu.VMEM((NSLOT, hid, inter), BF16),
                pltpu.VMEM((NCACHE, GROUP, kvd, lmax), BF16),
                pltpu.VMEM(w_dkv.shape[::-1], BF16),
                pltpu.VMEM(w_uk.shape, BF16),
                pltpu.VMEM(w_uv.shape, BF16),
                pltpu.VMEM((bsz, w_q.shape[1]), BF16),
                pltpu.VMEM((kvl // 128 + 1, bsz * heads, 128), F32),
                pltpu.VMEM((bsz, kvl + 128), F32),
                pltpu.VMEM((bsz, hid), BF16),
                pltpu.VMEM((bsz, hid), BF16),
                pltpu.VMEM((nt, hid), BF16),
                pltpu.VMEM((nt, 128), F32),
                pltpu.VMEM((n_loc * rows_e, nt), BF16),
                pltpu.VMEM((3, nt, n_loc * rows_e), BF16),
                pltpu.VMEM((rows_e, hid), BF16),
                pltpu.VMEM((n_loc * rows_e, inter), BF16),
                pltpu.VMEM((bsz, 2 * inter), BF16),
                pltpu.VMEM((n_loc * rows_e, cw), BF16),
                pltpu.VMEM((2, hid // 128, bsz, 128), F32),
                pltpu.VMEM((hid // 128, bsz, 128), F32),
                pltpu.VMEM((hid // 128, bsz, 128), F32),
                pltpu.VMEM((bsz, hid), F32),
                dma((NSLOT,)), dma((NCACHE,)), dma((3,)),
                dma((n - 1,)), dma((n - 1,)), dma((3,)), dma((3,)),
                dma((NCHUNK, 2)), dma((NCHUNK, 2)), dma((NCHUNK,)), dma((NCHUNK,)),
            ],
            compiler_params=pltpu.CompilerParams(collective_id=0, has_side_effects=True, vmem_limit_bytes=67_043_328),
        )
        return call(lens, lens.reshape(1, bsz), inv, x, ids.T, rw.T, cache.transpose(0, 2, 1), w_q, w_dkv.T, w_uk, w_uv, w_o,
                    s_gate, s_up, s_down, e_gate, e_up, e_down)

    in_specs = (row_spec, cache_spec, tok_spec, row_spec, row_spec) + (P(),) * 8 + (exp_spec,) * 3
    return jax.shard_map(local, mesh=mesh, in_specs=in_specs, out_specs=(row_spec, row_spec), check_vma=False)
```

```python
import math

import numpy as np
import jax
import jax.numpy as jnp
from jax import lax
from jax.experimental import pallas as pl
from jax.experimental.pallas import tpu as pltpu
from jax.sharding import PartitionSpec as P

EPS = 1e-6
ROPE_BASE = 1.0e4
CAP_FACTOR = 2
F32 = jnp.float32
BF16 = jnp.bfloat16
NSLOT = 6
NCACHE = 5
GROUP = 8
CHUNKS = (640, 640, 512, 256)
MESH = pl.DeviceIdType.MESH


def dot(a, b):
    return jnp.dot(a, b, preferred_element_type=F32)


def dot_nt(a, b):
    return lax.dot_general(a, b, (((1,), (1,)), ((), ())), preferred_element_type=F32)


def rms(v):
    return v * lax.rsqrt(jnp.mean(v * v, axis=-1, keepdims=True) + EPS)


def silu(g):
    return g / (1.0 + jnp.exp(-g))


def tiles(width, step):
    return [(a, min(step, width - a)) for a in range(0, width, step)]


def iota(shape, dim):
    return lax.broadcasted_iota(jnp.int32, shape, dim)


def layer_kernel(cape, lens, lens_row, inv_h, x_h, ids_h, rw_h, cache, w_q, w_dkv, w_uk, w_uv, w_o, s_gate, s_up, s_down, e_gate, e_up, e_down,
                 y, kvn,
                 lens_s, lens_v, inv, x, ids, rw, ring, cbuf, uk_b, uv_b, q_s, qf, kv_s, o_s, h1_s, u_all, gw_all, d_s, w_s, xr, acts, acts_sh, outs, rp, xs, rc, sh,
                 in_sem, q_sem, ring_sem, c_sem, w_sem, gw_send, gw_recv, u_send, u_recv, p_send, p_recv, x_send, x_recv):
    bsz, hid = x.shape
    heads, nope, kvl = w_uk.shape
    kvd, lmax = cache.shape[1:]
    qkd = nope + kvd - kvl
    vh = w_uv.shape[2]
    n_loc = e_gate.shape[0]
    inter = e_gate.shape[2]
    n_dev = gw_all.shape[0] // bsz
    rows_e = n_dev * cape
    grows = GROUP * heads
    nlat = kvl // 128
    nch = len(CHUNKS)
    starts = [sum(CHUNKS[:j]) for j in range(nch)]
    me = lax.axis_index("ep")

    def peer(k):
        return jnp.bitwise_xor(me, k)

    barrier = pltpu.get_barrier_semaphore()
    for k in range(1, n_dev):
        pl.semaphore_signal(barrier, inc=1, device_id={"ep": peer(k)}, device_id_type=MESH)

    def to_slot(src, slot, rows=None, cols=None):
        dst = ring.at[slot]
        if rows is not None:
            dst = ring.at[slot, pl.ds(0, rows), pl.ds(0, cols)]
        return pltpu.make_async_copy(src, dst, ring_sem.at[slot])

    wq_cols = []
    for i in range(3):
        for b, w in tiles(min(inter, w_q.shape[1] - i * inter), 768):
            wq_cols.append((i, b, w))

    def wq_job(p):
        i, b, w = wq_cols[p]
        return pltpu.make_async_copy(w_q.at[:, pl.ds(i * inter + b, w)], ring.at[i, :, pl.ds(b, w)], q_sem.at[p])

    def wo_job(i):
        a = i * inter
        w = min(inter, hid - a)
        return to_slot(w_o.at[:, pl.ds(a, w)], 3 + i, heads * vh, w)

    def sgu_job(i):
        src = s_gate if i % 2 == 0 else s_up
        return to_slot(src.at[:, pl.ds((i // 2) * inter, inter)], (5 + i) % NSLOT)

    def gate_job(e):
        return to_slot(e_gate.at[e], lax.rem(9 + 2 * e, NSLOT))

    def up_job(e):
        return to_slot(e_up.at[e], lax.rem(10 + 2 * e, NSLOT))

    def down_job(j, e):
        slot = lax.rem(41 + j * n_loc + e, NSLOT)
        return to_slot(e_down.at[e, :, pl.ds(starts[j], CHUNKS[j])], slot, inter, CHUNKS[j])

    def sd_job(i):
        r = i % 2
        c = i // 2
        half = hid // 2
        return to_slot(s_down.at[pl.ds(r * inter, inter), pl.ds(c * half, half)], (105 + i) % NSLOT, inter, half)

    def cache_job(g):
        s = lax.rem(g, NCACHE)
        return pltpu.make_async_copy(cache.at[pl.ds(g * GROUP, GROUP)], cbuf.at[s], c_sem.at[s])

    dkv_a = inter - 256
    dkv_copies = [pltpu.make_async_copy(w_dkv.at[:, pl.ds(0, dkv_a)], ring.at[2, pl.ds(0, kvd), pl.ds(256, dkv_a)], w_sem.at[0]),
                  pltpu.make_async_copy(w_dkv.at[:, pl.ds(dkv_a, hid - dkv_a)], ring.at[2, pl.ds(kvd, kvd), pl.ds(256, hid - dkv_a)], w_sem.at[3])]
    uk_copy = pltpu.make_async_copy(w_uk, uk_b, w_sem.at[1])
    uv_copy = pltpu.make_async_copy(w_uv, uv_b, w_sem.at[2])
    small = [pltpu.make_async_copy(a, b, in_sem.at[i]) for i, (a, b) in enumerate(
        ((x_h, x), (lens, lens_s), (lens_row, lens_v), (inv_h, inv), (ids_h, ids), (rw_h, rw)))]
    for c in small:
        c.start()
    for p in range(3):
        wq_job(p).start()
    for c in small:
        c.wait()

    col = iota((bsz, 128), 1)
    expert = iota((128, bsz), 0)
    gw = jnp.zeros((128, bsz), F32)
    for k in range(ids.shape[0]):
        gw = gw + jnp.where(ids[k:k + 1, :] == expert, rw[k:k + 1, :], 0.0)
    gw_all[pl.ds(pl.multiple_of(me * bsz, bsz), bsz), :] = gw.T

    diag = iota((bsz, bsz), 0) == iota((bsz, bsz), 1)
    pos = jnp.sum(jnp.where(diag, jnp.broadcast_to(lens_v[...], (bsz, bsz)), 0), axis=1, keepdims=True).astype(F32)
    ang = pos * inv[...]
    cs = jnp.cos(ang)
    half = (kvd - kvl) // 2
    low = col < half
    sn = jnp.where(low, -1.0, 1.0) * jnp.sin(ang)

    def rope(v):
        sw = jnp.where(low, pltpu.roll(v, 128 - half, 1), pltpu.roll(v, half, 1))
        return v * cs + sw * sn

    xf = x[...].astype(F32)
    xn = rms(xf).astype(BF16)

    pl.semaphore_wait(barrier, n_dev - 1)

    def gw_copy(k):
        mine = gw_all.at[pl.ds(pl.multiple_of(me * bsz, bsz), bsz)]
        return pltpu.make_async_remote_copy(mine, mine, gw_send.at[k - 1], gw_recv.at[k - 1], device_id={"ep": peer(k)}, device_id_type=MESH)

    for k in range(1, n_dev):
        gw_copy(k).start()

    following = [[wq_job(3)], [wq_job(4)] + dkv_copies, [uk_copy, cache_job(0)], [cache_job(1)], [cache_job(2)]]
    for p, (i, b, w) in enumerate(wq_cols):
        wq_job(p).wait()
        for c in following[p]:
            c.start()
        a = i * inter + b
        q_s[:, a:a + w] = dot(xn, ring[i, :, b:b + w]).astype(BF16)
    for c in dkv_copies:
        c.wait()
    kv = dot_nt(xn[:, :dkv_a], ring[2, :kvd, 256:]) + dot_nt(xn[:, dkv_a:], ring[2, kvd:2 * kvd, 256:256 + hid - dkv_a])
    kv_s[...] = jnp.zeros_like(kv_s)
    kv_s[:, :kvd] = kv
    kvn[:, :kvl] = rms(kv_s[:, :kvl]).astype(BF16)
    kvn[:, kvl:] = rope(kv_s[:, kvl:kvl + 128])[:, :kvd - kvl].astype(BF16)

    uk_copy.wait()
    cache_job(3).start()
    left = col < 64

    def put_head(h, q_nope, q_rot):
        ql = dot(q_nope.astype(BF16), uk_b[h])
        for c in range(nlat):
            qf[c, pl.ds(h, bsz, stride=heads), :] = ql[:, 128 * c:128 * (c + 1)]
        qf[nlat, pl.ds(h, bsz, stride=heads), :] = jnp.where(left, rope(q_rot), 0.0)

    for hp in range(heads // 2):
        a = hp * 2 * qkd
        b0 = q_s[:, a:a + 128].astype(F32)
        b1 = q_s[:, a + 128:a + 256].astype(F32)
        b2 = q_s[:, a + 256:a + 384].astype(F32)
        r1 = pltpu.roll(b1, 64, 1)
        r2 = pltpu.roll(b2, 64, 1)
        put_head(2 * hp, b0, b1)
        put_head(2 * hp + 1, jnp.where(left, r1, r2), r2)

    scale = qkd ** -0.5
    n_groups = bsz // GROUP
    tpos = iota((heads, lmax), 1)
    seq_of_row = iota((grows, bsz), 0) // heads
    seq_col = iota((grows, bsz), 1)

    def attend(g, carry):
        s = lax.rem(g, NCACHE)
        cache_job(g).wait()

        @pl.when(g + 4 < n_groups)
        def _():
            cache_job(g + 4).start()

        for k, group in enumerate(([uv_copy, wo_job(0)], [wo_job(1)], [sgu_job(0)], [sgu_job(1)])):
            @pl.when(g == n_groups - 4 + k)
            def _():
                for c in group:
                    c.start()
        rows = pl.ds(pl.multiple_of(g * grows, grows), grows)
        qg = jnp.concatenate([qf[c, rows, :].astype(BF16) for c in range(nlat + 1)], axis=1)[:, :kvd]
        own = seq_col == seq_of_row + g * GROUP
        s_new = jnp.sum(jnp.where(own, dot_nt(qg, kvn[...]), 0.0), axis=1, keepdims=True) * scale
        parts = []
        for i in range(GROUP):
            si = dot(qg[i * heads:(i + 1) * heads], cbuf[s, i]) * scale
            parts.append(jnp.where(tpos < lens_s[g * GROUP + i], si, -jnp.inf))
        sc = jnp.concatenate(parts, axis=0)
        mx = jnp.maximum(jnp.max(sc, axis=1, keepdims=True), s_new)
        e = jnp.exp(sc - mx)
        e_new = jnp.exp(s_new - mx)
        den = jnp.sum(e, axis=1, keepdims=True) + e_new
        rden = 1.0 / den
        p = (e * rden).astype(BF16)
        p_new = jnp.where(own, e_new * rden, 0.0).astype(BF16)
        o_new = dot(p_new, kvn[:, :kvl])
        outs_i = [dot_nt(p[i * heads:(i + 1) * heads], cbuf[s, i, :kvl, :]) for i in range(GROUP)]
        o_lat = jnp.concatenate(outs_i, axis=0) + o_new
        for c in range(nlat):
            qf[c, rows, :] = o_lat[:, 128 * c:128 * (c + 1)]
        return carry

    lax.fori_loop(0, n_groups, attend, 0)
    sgu_job(2).start()
    uv_copy.wait()
    sgu_job(3).start()
    for h in range(heads):
        oh = jnp.concatenate([qf[c, pl.ds(h, bsz, stride=heads), :].astype(BF16) for c in range(nlat)], axis=1)
        o_s[:, h * vh:(h + 1) * vh] = dot(oh, uv_b[h]).astype(BF16)
    for i in range(2):
        wo_job(i).wait()
        a = i * inter
        for b, w in tiles(min(inter, hid - a), 512):
            h1_s[:, a + b:a + b + w] = (x[:, a + b:a + b + w].astype(F32) + dot(o_s[...], ring[3 + i, :, b:b + w])).astype(BF16)
    gate_job(0).start()
    up_job(0).start()

    u = rms(h1_s[...].astype(F32)).astype(BF16)
    mine = pl.ds(pl.multiple_of(me * bsz, bsz), bsz)
    across = pl.ds(pl.multiple_of(peer(2) * bsz, bsz), bsz)
    u_all[mine, :] = u

    def u_copy(rows, i, k):
        blk = u_all.at[rows]
        return pltpu.make_async_remote_copy(blk, blk, u_send.at[i], u_recv.at[i], device_id={"ep": peer(k)}, device_id_type=MESH)

    u_copy(mine, 1, 2).start()
    u_copy(mine, 0, 1).start()

    def shared_gu(i):
        for j in range(2):
            sgu_job(2 * i + j).wait()
        uu = u_all[mine, :]
        for b, w in tiles(inter, 512):
            gg = dot(uu, ring[(5 + 2 * i) % NSLOT, :, b:b + w])
            vv = dot(uu, ring[(6 + 2 * i) % NSLOT, :, b:b + w])
            acts_sh[:, i * inter + b:i * inter + b + w] = (silu(gg) * vv).astype(BF16)

    shared_gu(0)
    gate_job(1).start()
    up_job(1).start()
    shared_gu(1)
    gate_job(2).start()
    up_job(2).start()

    for k in range(1, n_dev):
        gw_copy(k).wait()
    nt = n_dev * bsz
    ga = gw_all[...]
    hit = ga > 0.0
    ti = iota((nt, nt), 0)
    tj = iota((nt, nt), 1)
    before = ((ti // bsz == tj // bsz) & (tj < ti)).astype(F32).astype(BF16)
    rank = dot(before, jnp.where(hit, 1.0, 0.0).astype(BF16))
    src = (iota((nt, 128), 0) // bsz * cape).astype(F32)
    code = jnp.where(hit, src + rank, -1.0)
    exp_r = iota((128, n_loc * rows_e), 0)
    exp_c = iota((128, n_loc * rows_e), 1) // rows_e
    spread = (exp_r == exp_c + me * n_loc).astype(F32).astype(BF16)
    code_x = dot(code.astype(BF16), spread)
    slot_c = (iota((nt, n_loc * rows_e), 1) % rows_e).astype(F32)
    member = code_x == slot_c
    g1 = ga.astype(BF16)
    res = ga - g1.astype(F32)
    g2 = res.astype(BF16)
    g3 = (res - g2.astype(F32)).astype(BF16)
    for t, gt in enumerate((g1, g2, g3)):
        w_s[t] = jnp.where(member, dot(gt, spread), 0.0).astype(BF16)
    d_s[...] = jnp.where(member, 1.0, 0.0).T.astype(BF16)

    u_copy(mine, 1, 2).wait_recv()
    u_copy(across, 2, 1).start()
    u_copy(mine, 0, 1).wait()
    u_copy(across, 2, 1).wait()
    u_copy(mine, 1, 2).wait_send()

    def gate_up(e, carry):
        erows = pl.ds(pl.multiple_of(e * rows_e, rows_e), rows_e)
        de = d_s[erows, :]
        for b, w in tiles(hid, 512):
            xr[:, b:b + w] = dot(de, u_all[:, b:b + w]).astype(BF16)
        gate_job(e).wait()
        up_job(e).wait()
        sg = lax.rem(9 + 2 * e, NSLOT)
        su = lax.rem(10 + 2 * e, NSLOT)
        for b, w in tiles(inter, 512):
            gg = dot(xr[...], ring[sg, :, b:b + w])
            vv = dot(xr[...], ring[su, :, b:b + w])
            acts[erows, b:b + w] = (silu(gg) * vv).astype(BF16)

        @pl.when(e + 3 < n_loc)
        def _():
            gate_job(e + 3).start()
            up_job(e + 3).start()

        @pl.when(e + 3 >= n_loc)
        def _():
            down_job(0, 2 * (e + 3 - n_loc)).start()
            down_job(0, 2 * (e + 3 - n_loc) + 1).start()
        return carry

    lax.fori_loop(0, n_loc, gate_up, 0)

    def part(j, d):
        return pl.ds(pl.multiple_of(j * nt + d * bsz, bsz), bsz)

    def blocks(j):
        return range(starts[j] // 128, (starts[j] + CHUNKS[j]) // 128)

    def pair_copy(j, i, d):
        return pltpu.make_async_remote_copy(qf.at[pl.ds(0, len(blocks(j))), part(j, d)], rp.at[i, pl.ds(blocks(j)[0], len(blocks(j)))],
                                            p_send.at[j, i], p_recv.at[j, i], device_id={"ep": peer(1)}, device_id_type=MESH)

    def cross_copy(j):
        blk = pl.ds(blocks(j)[0], len(blocks(j)))
        return pltpu.make_async_remote_copy(xs.at[blk], rc.at[blk], x_send.at[j], x_recv.at[j],
                                            device_id={"ep": peer(2)}, device_id_type=MESH)

    def start_pair(j):
        pair_copy(j, 1, peer(3)).start()
        pair_copy(j, 0, peer(1)).start()

    def forward(j):
        pair_copy(j, 1, peer(3)).wait_recv()
        for c, b in enumerate(blocks(j)):
            xs[b] = qf[c, part(j, peer(2)), :] + rp[1, b]
        cross_copy(j).start()

    for j in range(nch):
        cw = CHUNKS[j]

        def down(e, carry):
            down_job(j, e).wait()
            erows = pl.ds(pl.multiple_of(e * rows_e, rows_e), rows_e)
            slot = lax.rem(41 + j * n_loc + e, NSLOT)
            outs[erows, :cw] = dot(acts[erows, :], ring[slot, :inter, :cw]).astype(BF16)

            @pl.when(e + NSLOT < n_loc)
            def _():
                down_job(j, e + NSLOT).start()

            if j < nch - 1:
                @pl.when(e + NSLOT >= n_loc)
                def _():
                    down_job(j + 1, e + NSLOT - n_loc).start()
            else:
                for k in range(4):
                    @pl.when(e == n_loc - NSLOT + k)
                    def _():
                        sd_job(k).start()
            return carry

        lax.fori_loop(0, n_loc, down, 0)
        if j >= 1:
            forward(j - 1)
        ov = outs[:, :cw]
        total = dot(w_s[0], ov) + dot(w_s[1], ov) + dot(w_s[2], ov)
        for c in range(cw // 128):
            qf[c, pl.ds(j * nt, nt), :] = total[:, 128 * c:128 * (c + 1)]
        start_pair(j)
    forward(nch - 1)

    hw = hid // 2
    for c in range(2):
        for r in range(2):
            sd_job(2 * c + r).wait()
        for b, w in tiles(hw, 512):
            acc = dot(acts_sh[:, :inter], ring[(105 + 2 * c) % NSLOT, :inter, b:b + w])
            acc += dot(acts_sh[:, inter:], ring[(106 + 2 * c) % NSLOT, :inter, b:b + w])
            sh[:, c * hw + b:c * hw + b + w] = acc

    for j in range(nch):
        pair_copy(j, 0, peer(1)).wait_recv()
        cross_copy(j).wait_recv()
        for c, b in enumerate(blocks(j)):
            cols = slice(b * 128, (b + 1) * 128)
            routed = qf[c, part(j, me), :] + rp[0, b] + rc[b]
            y[:, cols] = (h1_s[:, cols].astype(F32) + sh[:, cols] + routed).astype(BF16)
    for j in range(nch):
        pair_copy(j, 1, peer(3)).wait_send()
        pair_copy(j, 0, peer(1)).wait_send()
        cross_copy(j).wait_send()


def solution(mesh):
    n = mesh.shape['ep']
    tok_spec = P(('rep', 'ep'))
    row_spec = P(('rep', 'ep'), None)
    cache_spec = P(('rep', 'ep'), None, None)
    exp_spec = P('ep', None, None)

    def local(x, cache, lens, ids, rw, w_q, w_dkv, w_uk, w_uv, w_o, s_gate, s_up, s_down, e_gate, e_up, e_down):
        bsz, hid = x.shape
        heads, nope, kvl = w_uk.shape
        lmax, kvd = cache.shape[1:]
        n_loc, _, inter = e_gate.shape
        top = ids.shape[1]
        n_exp = n_loc * n
        cape = (CAP_FACTOR * bsz * top + n_exp - 1) // n_exp
        rows_e = n * cape
        nt = n * bsz
        half = (kvd - kvl) // 2
        inv = np.float64(ROPE_BASE) ** (-2.0 * (np.arange(128) % half) / (kvd - kvl))
        inv = jnp.asarray(inv.astype(np.float32)[None, :])
        vm = pl.BlockSpec(memory_space=pltpu.VMEM)
        hb = pl.BlockSpec(memory_space=pl.ANY)
        dma = pltpu.SemaphoreType.DMA
        call = pl.pallas_call(
            lambda *refs: layer_kernel(cape, *refs),
            name="layer",
            out_shape=(pltpu.VMEM((bsz, hid), BF16), pltpu.VMEM((bsz, kvd), BF16)),
            in_specs=[hb] * 18,
            out_specs=(vm, vm),
            scratch_shapes=[
                pltpu.SMEM((bsz,), jnp.int32),
                pltpu.VMEM((1, bsz), jnp.int32),
                pltpu.VMEM((1, 128), F32),
                pltpu.VMEM((bsz, hid), BF16),
                pltpu.VMEM((top, bsz), jnp.int32),
                pltpu.VMEM((top, bsz), F32),
                pltpu.VMEM((NSLOT, hid, inter), BF16),
                pltpu.VMEM((NCACHE, GROUP, kvd, lmax), BF16),
                pltpu.VMEM(w_uk.shape, BF16),
                pltpu.VMEM(w_uv.shape, BF16),
                pltpu.VMEM((bsz, w_q.shape[1]), BF16),
                pltpu.VMEM((kvl // 128 + 1, bsz * heads, 128), F32),
                pltpu.VMEM((bsz, kvl + 128), F32),
                pltpu.VMEM((bsz, hid), BF16),
                pltpu.VMEM((bsz, hid), BF16),
                pltpu.VMEM((nt, hid), BF16),
                pltpu.VMEM((nt, 128), F32),
                pltpu.VMEM((n_loc * rows_e, nt), BF16),
                pltpu.VMEM((3, nt, n_loc * rows_e), BF16),
                pltpu.VMEM((rows_e, hid), BF16),
                pltpu.VMEM((n_loc * rows_e, inter), BF16),
                pltpu.VMEM((bsz, 2 * inter), BF16),
                pltpu.VMEM((n_loc * rows_e, max(CHUNKS)), BF16),
                pltpu.VMEM((2, hid // 128, bsz, 128), F32),
                pltpu.VMEM((hid // 128, bsz, 128), F32),
                pltpu.VMEM((hid // 128, bsz, 128), F32),
                pltpu.VMEM((bsz, hid), F32),
                dma((6,)), dma((5,)), dma((NSLOT,)), dma((NCACHE,)), dma((4,)),
                dma((n - 1,)), dma((n - 1,)), dma((3,)), dma((3,)),
                dma((len(CHUNKS), 2)), dma((len(CHUNKS), 2)), dma((len(CHUNKS),)), dma((len(CHUNKS),)),
            ],
            compiler_params=pltpu.CompilerParams(collective_id=0, has_side_effects=True, vmem_limit_bytes=66_600_000),
        )
        return call(lens, lens.reshape(1, bsz), inv, x, ids.T, rw.T, cache.transpose(0, 2, 1), w_q, w_dkv.T, w_uk, w_uv, w_o,
                    s_gate, s_up, s_down, e_gate, e_up, e_down)

    in_specs = (row_spec, cache_spec, tok_spec, row_spec, row_spec) + (P(),) * 8 + (exp_spec,) * 3
    return jax.shard_map(local, mesh=mesh, in_specs=in_specs, out_specs=(row_spec, row_spec), check_vma=False)
```

```python
import math

import numpy as np
import jax
import jax.numpy as jnp
from jax import lax
from jax.experimental import pallas as pl
from jax.experimental.pallas import tpu as pltpu
from jax.sharding import PartitionSpec as P

EPS = 1e-6
ROPE_BASE = 1.0e4
CAP_FACTOR = 2
F32 = jnp.float32
BF16 = jnp.bfloat16
NSLOT = 6
NCACHE = 5
GROUP = 8
CHUNKS = (640, 640, 384, 256, 128)
PACK = (1, 1, 2, 2, 4)
PLACE = ((0, 0), (1, 0), (2, 0), (3, 0), (3, 2))
MESH = pl.DeviceIdType.MESH


def dot(a, b):
    return jnp.dot(a, b, preferred_element_type=F32)


def dot_nt(a, b):
    return lax.dot_general(a, b, (((1,), (1,)), ((), ())), preferred_element_type=F32)


def rms(v):
    return v * lax.rsqrt(jnp.mean(v * v, axis=-1, keepdims=True) + EPS)


def silu(g):
    return g / (1.0 + jnp.exp(-g))


def tiles(width, step):
    return [(a, min(step, width - a)) for a in range(0, width, step)]


def iota(shape, dim):
    return lax.broadcasted_iota(jnp.int32, shape, dim)


def layer_kernel(cape, lens, lens_row, inv_h, x_h, ids_h, rw_h, cache, w_q, w_dkv, w_uk, w_uv, w_o, s_gate, s_up, s_down, e_gate, e_up, e_down,
                 y, kvn,
                 lens_s, lens_v, inv, x, ids, rw, ring, cbuf, uk_b, uv_b, q_s, qf, kv_s, o_s, h1_s, u_all, gw_all, d_s, w_s, xr, acts, acts_sh, outs, rp, xs, rc, sh,
                 in_sem, q_sem, ring_sem, d_sem, c_sem, w_sem, gw_send, gw_recv, u_send, u_recv, p_send, p_recv, x_send, x_recv):
    bsz, hid = x.shape
    heads, nope, kvl = w_uk.shape
    kvd, lmax = cache.shape[1:]
    qkd = nope + kvd - kvl
    vh = w_uv.shape[2]
    n_loc = e_gate.shape[0]
    inter = e_gate.shape[2]
    n_dev = gw_all.shape[0] // bsz
    rows_e = n_dev * cape
    grows = GROUP * heads
    nlat = kvl // 128
    nch = len(CHUNKS)
    starts = [sum(CHUNKS[:j]) for j in range(nch)]
    n_jobs = [n_loc // p for p in PACK]
    base = [sum(n_jobs[:j]) for j in range(nch + 1)]
    sd_base = 41 + base[nch]
    me = lax.axis_index("ep")

    def peer(k):
        return jnp.bitwise_xor(me, k)

    barrier = pltpu.get_barrier_semaphore()
    for k in range(1, n_dev):
        pl.semaphore_signal(barrier, inc=1, device_id={"ep": peer(k)}, device_id_type=MESH)

    def to_slot(src, slot, rows=None, cols=None):
        dst = ring.at[slot]
        if rows is not None:
            dst = ring.at[slot, pl.ds(0, rows), pl.ds(0, cols)]
        return pltpu.make_async_copy(src, dst, ring_sem.at[slot])

    wq_cols = []
    for i in range(3):
        for b, w in tiles(min(inter, w_q.shape[1] - i * inter), 768):
            wq_cols.append((i, b, w))

    def wq_job(p):
        i, b, w = wq_cols[p]
        return pltpu.make_async_copy(w_q.at[:, pl.ds(i * inter + b, w)], ring.at[i, :, pl.ds(b, w)], q_sem.at[p])

    def wo_job(i):
        a = i * inter
        w = min(inter, hid - a)
        return to_slot(w_o.at[:, pl.ds(a, w)], 3 + i, heads * vh, w)

    def sgu_job(i):
        src = s_gate if i % 2 == 0 else s_up
        return to_slot(src.at[:, pl.ds((i // 2) * inter, inter)], (5 + i) % NSLOT)

    def gate_job(e):
        return to_slot(e_gate.at[e], lax.rem(9 + 2 * e, NSLOT))

    def up_job(e):
        return to_slot(e_up.at[e], lax.rem(10 + 2 * e, NSLOT))

    def down_job(j, t):
        slot = lax.rem(41 + base[j] + t, NSLOT)
        return [pltpu.make_async_copy(e_down.at[t * PACK[j] + q, :, pl.ds(starts[j], CHUNKS[j])],
                                      ring.at[slot, pl.ds(0, inter), pl.ds(q * CHUNKS[j], CHUNKS[j])],
                                      ring_sem.at[slot] if PACK[j] == 1 else d_sem.at[slot, q]) for q in range(PACK[j])]

    def start_down(j, t):
        for c in down_job(j, t):
            c.start()

    def sd_job(i):
        r = i % 2
        c = i // 2
        half = hid // 2
        return to_slot(s_down.at[pl.ds(r * inter, inter), pl.ds(c * half, half)], (sd_base + i) % NSLOT, inter, half)

    def cache_job(g):
        s = lax.rem(g, NCACHE)
        return pltpu.make_async_copy(cache.at[pl.ds(g * GROUP, GROUP)], cbuf.at[s], c_sem.at[s])

    dkv_a = inter - 256
    dkv_copies = [pltpu.make_async_copy(w_dkv.at[:, pl.ds(0, dkv_a)], ring.at[2, pl.ds(0, kvd), pl.ds(256, dkv_a)], w_sem.at[0]),
                  pltpu.make_async_copy(w_dkv.at[:, pl.ds(dkv_a, hid - dkv_a)], ring.at[2, pl.ds(kvd, kvd), pl.ds(256, hid - dkv_a)], w_sem.at[3])]
    uk_copy = pltpu.make_async_copy(w_uk, uk_b, w_sem.at[1])
    uv_copy = pltpu.make_async_copy(w_uv, uv_b, w_sem.at[2])
    small = [pltpu.make_async_copy(a, b, in_sem.at[i]) for i, (a, b) in enumerate(
        ((x_h, x), (lens, lens_s), (lens_row, lens_v), (inv_h, inv), (ids_h, ids), (rw_h, rw)))]
    for c in small:
        c.start()
    for p in range(3):
        wq_job(p).start()
    for c in small:
        c.wait()

    col = iota((bsz, 128), 1)
    expert = iota((128, bsz), 0)
    gw = jnp.zeros((128, bsz), F32)
    for k in range(ids.shape[0]):
        gw = gw + jnp.where(ids[k:k + 1, :] == expert, rw[k:k + 1, :], 0.0)
    gw_all[pl.ds(pl.multiple_of(me * bsz, bsz), bsz), :] = gw.T

    diag = iota((bsz, bsz), 0) == iota((bsz, bsz), 1)
    pos = jnp.sum(jnp.where(diag, jnp.broadcast_to(lens_v[...], (bsz, bsz)), 0), axis=1, keepdims=True).astype(F32)
    ang = pos * inv[...]
    cs = jnp.cos(ang)
    half = (kvd - kvl) // 2
    low = col < half
    sn = jnp.where(low, -1.0, 1.0) * jnp.sin(ang)

    def rope(v):
        sw = jnp.where(low, pltpu.roll(v, 128 - half, 1), pltpu.roll(v, half, 1))
        return v * cs + sw * sn

    xf = x[...].astype(F32)
    xn = rms(xf).astype(BF16)

    pl.semaphore_wait(barrier, n_dev - 1)

    def gw_copy(k):
        mine = gw_all.at[pl.ds(pl.multiple_of(me * bsz, bsz), bsz)]
        return pltpu.make_async_remote_copy(mine, mine, gw_send.at[k - 1], gw_recv.at[k - 1], device_id={"ep": peer(k)}, device_id_type=MESH)

    for k in range(1, n_dev):
        gw_copy(k).start()

    following = [[wq_job(3)], [wq_job(4)] + dkv_copies, [uk_copy, cache_job(0)], [cache_job(1)], [cache_job(2)]]
    for p, (i, b, w) in enumerate(wq_cols):
        wq_job(p).wait()
        for c in following[p]:
            c.start()
        a = i * inter + b
        q_s[:, a:a + w] = dot(xn, ring[i, :, b:b + w]).astype(BF16)
    for c in dkv_copies:
        c.wait()
    kv = dot_nt(xn[:, :dkv_a], ring[2, :kvd, 256:]) + dot_nt(xn[:, dkv_a:], ring[2, kvd:2 * kvd, 256:256 + hid - dkv_a])
    kv_s[...] = jnp.zeros_like(kv_s)
    kv_s[:, :kvd] = kv
    kvn[:, :kvl] = rms(kv_s[:, :kvl]).astype(BF16)
    kvn[:, kvl:] = rope(kv_s[:, kvl:kvl + 128])[:, :kvd - kvl].astype(BF16)

    uk_copy.wait()
    cache_job(3).start()
    left = col < 64

    def put_head(h, q_nope, q_rot):
        ql = dot(q_nope.astype(BF16), uk_b[h])
        for c in range(nlat):
            qf[c, pl.ds(h, bsz, stride=heads), :] = ql[:, 128 * c:128 * (c + 1)]
        qf[nlat, pl.ds(h, bsz, stride=heads), :] = jnp.where(left, rope(q_rot), 0.0)

    for hp in range(heads // 2):
        a = hp * 2 * qkd
        b0 = q_s[:, a:a + 128].astype(F32)
        b1 = q_s[:, a + 128:a + 256].astype(F32)
        b2 = q_s[:, a + 256:a + 384].astype(F32)
        r1 = pltpu.roll(b1, 64, 1)
        r2 = pltpu.roll(b2, 64, 1)
        put_head(2 * hp, b0, b1)
        put_head(2 * hp + 1, jnp.where(left, r1, r2), r2)

    scale = qkd ** -0.5
    n_groups = bsz // GROUP
    tpos = iota((heads, lmax), 1)
    seq_of_row = iota((grows, bsz), 0) // heads
    seq_col = iota((grows, bsz), 1)

    def attend(g, carry):
        s = lax.rem(g, NCACHE)
        cache_job(g).wait()

        @pl.when(g + 4 < n_groups)
        def _():
            cache_job(g + 4).start()

        for k, group in enumerate(([uv_copy], [wo_job(1)], [wo_job(0)], [sgu_job(0)], [sgu_job(1)], [sgu_job(2)], [sgu_job(3)])):
            @pl.when(g == k)
            def _():
                for c in group:
                    c.start()
        rows = pl.ds(pl.multiple_of(g * grows, grows), grows)
        qg = jnp.concatenate([qf[c, rows, :].astype(BF16) for c in range(nlat + 1)], axis=1)[:, :kvd]
        own = seq_col == seq_of_row + g * GROUP
        s_new = jnp.sum(jnp.where(own, dot_nt(qg, kvn[...]), 0.0), axis=1, keepdims=True) * scale
        parts = []
        for i in range(GROUP):
            si = dot(qg[i * heads:(i + 1) * heads], cbuf[s, i]) * scale
            parts.append(jnp.where(tpos < lens_s[g * GROUP + i], si, -jnp.inf))
        sc = jnp.concatenate(parts, axis=0)
        mx = jnp.maximum(jnp.max(sc, axis=1, keepdims=True), s_new)
        e = jnp.exp(sc - mx)
        e_new = jnp.exp(s_new - mx)
        den = jnp.sum(e, axis=1, keepdims=True) + e_new
        rden = 1.0 / den
        p = (e * rden).astype(BF16)
        p_new = jnp.where(own, e_new * rden, 0.0).astype(BF16)
        o_new = dot(p_new, kvn[:, :kvl])
        outs_i = [dot_nt(p[i * heads:(i + 1) * heads], cbuf[s, i, :kvl, :]) for i in range(GROUP)]
        o_lat = jnp.concatenate(outs_i, axis=0) + o_new
        for c in range(nlat):
            qf[c, rows, :] = o_lat[:, 128 * c:128 * (c + 1)]
        return carry

    lax.fori_loop(0, n_groups, attend, 0)
    uv_copy.wait()
    for h in range(heads):
        oh = jnp.concatenate([qf[c, pl.ds(h, bsz, stride=heads), :].astype(BF16) for c in range(nlat)], axis=1)
        o_s[:, h * vh:(h + 1) * vh] = dot(oh, uv_b[h]).astype(BF16)
    for i in range(2):
        wo_job(i).wait()
        a = i * inter
        for b, w in tiles(min(inter, hid - a), 512):
            h1_s[:, a + b:a + b + w] = (x[:, a + b:a + b + w].astype(F32) + dot(o_s[...], ring[3 + i, :, b:b + w])).astype(BF16)
    gate_job(0).start()
    up_job(0).start()

    u = rms(h1_s[...].astype(F32)).astype(BF16)
    mine = pl.ds(pl.multiple_of(me * bsz, bsz), bsz)
    across = pl.ds(pl.multiple_of(peer(2) * bsz, bsz), bsz)
    u_all[mine, :] = u

    def u_copy(rows, i, k):
        blk = u_all.at[rows]
        return pltpu.make_async_remote_copy(blk, blk, u_send.at[i], u_recv.at[i], device_id={"ep": peer(k)}, device_id_type=MESH)

    u_copy(mine, 1, 2).start()
    u_copy(mine, 0, 1).start()

    def shared_gu(i):
        for j in range(2):
            sgu_job(2 * i + j).wait()
        uu = u_all[mine, :]
        for b, w in tiles(inter, 512):
            gg = dot(uu, ring[(5 + 2 * i) % NSLOT, :, b:b + w])
            vv = dot(uu, ring[(6 + 2 * i) % NSLOT, :, b:b + w])
            acts_sh[:, i * inter + b:i * inter + b + w] = (silu(gg) * vv).astype(BF16)

    shared_gu(0)
    gate_job(1).start()
    up_job(1).start()
    shared_gu(1)
    gate_job(2).start()
    up_job(2).start()

    for k in range(1, n_dev):
        gw_copy(k).wait()
    nt = n_dev * bsz
    ga = gw_all[...]
    hit = ga > 0.0
    ti = iota((nt, nt), 0)
    tj = iota((nt, nt), 1)
    before = ((ti // bsz == tj // bsz) & (tj < ti)).astype(F32).astype(BF16)
    rank = dot(before, jnp.where(hit, 1.0, 0.0).astype(BF16))
    src = (iota((nt, 128), 0) // bsz * cape).astype(F32)
    code = jnp.where(hit, src + rank, -1.0)
    exp_r = iota((128, n_loc * rows_e), 0)
    exp_c = iota((128, n_loc * rows_e), 1) // rows_e
    spread = (exp_r == exp_c + me * n_loc).astype(F32).astype(BF16)
    code_x = dot(code.astype(BF16), spread)
    slot_c = (iota((nt, n_loc * rows_e), 1) % rows_e).astype(F32)
    member = code_x == slot_c
    g1 = ga.astype(BF16)
    res = ga - g1.astype(F32)
    g2 = res.astype(BF16)
    g3 = (res - g2.astype(F32)).astype(BF16)
    for t, gt in enumerate((g1, g2, g3)):
        w_s[t] = jnp.where(member, dot(gt, spread), 0.0).astype(BF16)
    d_s[...] = jnp.where(member, 1.0, 0.0).T.astype(BF16)

    u_copy(mine, 1, 2).wait_recv()
    u_copy(across, 2, 1).start()
    u_copy(mine, 0, 1).wait()
    u_copy(across, 2, 1).wait()
    u_copy(mine, 1, 2).wait_send()

    def gate_up(e, carry):
        erows = pl.ds(pl.multiple_of(e * rows_e, rows_e), rows_e)
        de = d_s[erows, :]
        for b, w in tiles(hid, 512):
            xr[:, b:b + w] = dot(de, u_all[:, b:b + w]).astype(BF16)
        gate_job(e).wait()
        up_job(e).wait()
        sg = lax.rem(9 + 2 * e, NSLOT)
        su = lax.rem(10 + 2 * e, NSLOT)
        for b, w in tiles(inter, 512):
            gg = dot(xr[...], ring[sg, :, b:b + w])
            vv = dot(xr[...], ring[su, :, b:b + w])
            acts[erows, b:b + w] = (silu(gg) * vv).astype(BF16)

        @pl.when(e + 3 < n_loc)
        def _():
            gate_job(e + 3).start()
            up_job(e + 3).start()

        @pl.when(e + 3 >= n_loc)
        def _():
            start_down(0, 2 * (e + 3 - n_loc))
            start_down(0, 2 * (e + 3 - n_loc) + 1)
        return carry

    lax.fori_loop(0, n_loc, gate_up, 0)

    def part(j, d):
        return pl.ds(pl.multiple_of(PLACE[j][0] * nt + d * bsz, bsz), bsz)

    def blocks(j):
        return range(starts[j] // 128, (starts[j] + CHUNKS[j]) // 128)

    def pair_copy(j, i, d):
        return pltpu.make_async_remote_copy(qf.at[pl.ds(PLACE[j][1], len(blocks(j))), part(j, d)], rp.at[i, pl.ds(blocks(j)[0], len(blocks(j)))],
                                            p_send.at[j, i], p_recv.at[j, i], device_id={"ep": peer(1)}, device_id_type=MESH)

    def cross_copy(j):
        blk = pl.ds(blocks(j)[0], len(blocks(j)))
        return pltpu.make_async_remote_copy(xs.at[blk], rc.at[blk], x_send.at[j], x_recv.at[j],
                                            device_id={"ep": peer(2)}, device_id_type=MESH)

    def start_pair(j):
        pair_copy(j, 1, peer(3)).start()
        pair_copy(j, 0, peer(1)).start()

    def forward(j):
        pair_copy(j, 1, peer(3)).wait_recv()
        for c, b in enumerate(blocks(j)):
            xs[b] = qf[PLACE[j][1] + c, part(j, peer(2)), :] + rp[1, b]
        cross_copy(j).start()

    for j in range(nch):
        cw = CHUNKS[j]

        def down(t, carry):
            for c in down_job(j, t):
                c.wait()
            slot = lax.rem(41 + base[j] + t, NSLOT)
            for q in range(PACK[j]):
                erows = pl.ds(pl.multiple_of((t * PACK[j] + q) * rows_e, rows_e), rows_e)
                outs[erows, :cw] = dot(acts[erows, :], ring[slot, :inter, q * cw:(q + 1) * cw]).astype(BF16)
            for j2 in range(j, nch):
                first = base[j] + NSLOT - base[j2]
                if first + n_jobs[j] > 0 and first < n_jobs[j2]:
                    @pl.when((t + first >= 0) & (t + first < n_jobs[j2]))
                    def _():
                        start_down(j2, t + first)
            for k in range(4):
                if base[j] <= base[nch] + k - NSLOT < base[j + 1]:
                    @pl.when(t == base[nch] + k - NSLOT - base[j])
                    def _():
                        sd_job(k).start()
            if j >= 1:
                @pl.when(t == n_jobs[j] // 2)
                def _():
                    forward(j - 1)
            return carry

        lax.fori_loop(0, n_jobs[j], down, 0)
        ov = outs[:, :cw]
        total = dot(w_s[0], ov) + dot(w_s[1], ov) + dot(w_s[2], ov)
        for c in range(cw // 128):
            qf[PLACE[j][1] + c, pl.ds(PLACE[j][0] * nt, nt), :] = total[:, 128 * c:128 * (c + 1)]
        start_pair(j)
    forward(nch - 1)

    hw = hid // 2

    def finish(j):
        pair_copy(j, 0, peer(1)).wait_recv()
        cross_copy(j).wait_recv()
        for c, b in enumerate(blocks(j)):
            cols = slice(b * 128, (b + 1) * 128)
            routed = qf[PLACE[j][1] + c, part(j, me), :] + rp[0, b] + rc[b]
            y[:, cols] = (h1_s[:, cols].astype(F32) + sh[:, cols] + routed).astype(BF16)

    for k in range(4):
        c, r = k // 2, k % 2
        if k == 3:
            finish(0)
        sd_job(k).wait()
        for b, w in tiles(hw, 512):
            cols = slice(c * hw + b, c * hw + b + w)
            acc = dot(acts_sh[:, r * inter:(r + 1) * inter], ring[(sd_base + k) % NSLOT, :inter, b:b + w])
            sh[:, cols] = acc if r == 0 else sh[:, cols] + acc
    for j in range(1, nch):
        finish(j)
    for j in range(nch):
        pair_copy(j, 1, peer(3)).wait_send()
        pair_copy(j, 0, peer(1)).wait_send()
        cross_copy(j).wait_send()


def solution(mesh):
    n = mesh.shape['ep']
    tok_spec = P(('rep', 'ep'))
    row_spec = P(('rep', 'ep'), None)
    cache_spec = P(('rep', 'ep'), None, None)
    exp_spec = P('ep', None, None)

    def local(x, cache, lens, ids, rw, w_q, w_dkv, w_uk, w_uv, w_o, s_gate, s_up, s_down, e_gate, e_up, e_down):
        bsz, hid = x.shape
        heads, nope, kvl = w_uk.shape
        lmax, kvd = cache.shape[1:]
        n_loc, _, inter = e_gate.shape
        top = ids.shape[1]
        n_exp = n_loc * n
        cape = (CAP_FACTOR * bsz * top + n_exp - 1) // n_exp
        rows_e = n * cape
        nt = n * bsz
        half = (kvd - kvl) // 2
        inv = np.float64(ROPE_BASE) ** (-2.0 * (np.arange(128) % half) / (kvd - kvl))
        inv = jnp.asarray(inv.astype(np.float32)[None, :])
        vm = pl.BlockSpec(memory_space=pltpu.VMEM)
        hb = pl.BlockSpec(memory_space=pl.ANY)
        dma = pltpu.SemaphoreType.DMA
        call = pl.pallas_call(
            lambda *refs: layer_kernel(cape, *refs),
            name="layer",
            out_shape=(pltpu.VMEM((bsz, hid), BF16), pltpu.VMEM((bsz, kvd), BF16)),
            in_specs=[hb] * 18,
            out_specs=(vm, vm),
            scratch_shapes=[
                pltpu.SMEM((bsz,), jnp.int32),
                pltpu.VMEM((1, bsz), jnp.int32),
                pltpu.VMEM((1, 128), F32),
                pltpu.VMEM((bsz, hid), BF16),
                pltpu.VMEM((top, bsz), jnp.int32),
                pltpu.VMEM((top, bsz), F32),
                pltpu.VMEM((NSLOT, hid, inter), BF16),
                pltpu.VMEM((NCACHE, GROUP, kvd, lmax), BF16),
                pltpu.VMEM(w_uk.shape, BF16),
                pltpu.VMEM(w_uv.shape, BF16),
                pltpu.VMEM((bsz, w_q.shape[1]), BF16),
                pltpu.VMEM((kvl // 128 + 1, bsz * heads, 128), F32),
                pltpu.VMEM((bsz, kvl + 128), F32),
                pltpu.VMEM((bsz, hid), BF16),
                pltpu.VMEM((bsz, hid), BF16),
                pltpu.VMEM((nt, hid), BF16),
                pltpu.VMEM((nt, 128), F32),
                pltpu.VMEM((n_loc * rows_e, nt), BF16),
                pltpu.VMEM((3, nt, n_loc * rows_e), BF16),
                pltpu.VMEM((rows_e, hid), BF16),
                pltpu.VMEM((n_loc * rows_e, inter), BF16),
                pltpu.VMEM((bsz, 2 * inter), BF16),
                pltpu.VMEM((n_loc * rows_e, max(CHUNKS)), BF16),
                pltpu.VMEM((2, hid // 128, bsz, 128), F32),
                pltpu.VMEM((hid // 128, bsz, 128), F32),
                pltpu.VMEM((hid // 128, bsz, 128), F32),
                pltpu.VMEM((bsz, hid), F32),
                dma((6,)), dma((5,)), dma((NSLOT,)), dma((NSLOT, max(PACK))), dma((NCACHE,)), dma((4,)),
                dma((n - 1,)), dma((n - 1,)), dma((3,)), dma((3,)),
                dma((len(CHUNKS), 2)), dma((len(CHUNKS), 2)), dma((len(CHUNKS),)), dma((len(CHUNKS),)),
            ],
            compiler_params=pltpu.CompilerParams(collective_id=0, has_side_effects=True, vmem_limit_bytes=66_600_000),
        )
        return call(lens, lens.reshape(1, bsz), inv, x, ids.T, rw.T, cache.transpose(0, 2, 1), w_q, w_dkv.T, w_uk, w_uv, w_o,
                    s_gate, s_up, s_down, e_gate, e_up, e_down)

    in_specs = (row_spec, cache_spec, tok_spec, row_spec, row_spec) + (P(),) * 8 + (exp_spec,) * 3
    return jax.shard_map(local, mesh=mesh, in_specs=in_specs, out_specs=(row_spec, row_spec), check_vma=False)
```

```python
import math

import numpy as np
import jax
import jax.numpy as jnp
from jax import lax
from jax.experimental import pallas as pl
from jax.experimental.pallas import tpu as pltpu
from jax.sharding import PartitionSpec as P

EPS = 1e-6
ROPE_BASE = 1.0e4
CAP_FACTOR = 2
F32 = jnp.float32
BF16 = jnp.bfloat16
NSLOT = 6
NCACHE = 5
GROUP = 8
CHUNKS = (256, 640, 640, 384, 128)
PACK = (1, 1, 1, 2, 4)
PLACE = ((3, 0), (0, 0), (1, 0), (2, 0), (3, 2))
MESH = pl.DeviceIdType.MESH


def dot(a, b):
    return jnp.dot(a, b, preferred_element_type=F32)


def dot_nt(a, b):
    return lax.dot_general(a, b, (((1,), (1,)), ((), ())), preferred_element_type=F32)


def rms(v):
    return v * lax.rsqrt(jnp.mean(v * v, axis=-1, keepdims=True) + EPS)


def silu(g):
    return g / (1.0 + jnp.exp(-g))


def tiles(width, step):
    return [(a, min(step, width - a)) for a in range(0, width, step)]


def iota(shape, dim):
    return lax.broadcasted_iota(jnp.int32, shape, dim)


def layer_kernel(cape, lens, lens_row, inv_h, x_h, ids_h, rw_h, cache, w_q, w_dkv, w_uk, w_uv, w_o, s_gate, s_up, s_down, e_gate, e_up, e_down,
                 y, kvn,
                 lens_s, lens_v, inv, x, ids, rw, ring, cbuf, uk_b, uv_b, q_s, qf, kv_s, o_s, h1_s, u_all, gw_all, d_s, w_s, xr, acts, acts_sh, outs, rp, xs, rc, sh,
                 in_sem, q_sem, e_sem, ring_sem, d_sem, c_sem, w_sem, gw_send, gw_recv, u_send, u_recv, p_send, p_recv, x_send, x_recv):
    bsz, hid = x.shape
    heads, nope, kvl = w_uk.shape
    kvd = w_dkv.shape[0]
    lmax = cache.shape[1]
    qkd = nope + kvd - kvl
    vh = w_uv.shape[2]
    n_loc = e_gate.shape[0]
    inter = e_gate.shape[2]
    n_dev = gw_all.shape[0] // bsz
    rows_e = n_dev * cape
    grows = GROUP * heads
    nlat = kvl // 128
    nch = len(CHUNKS)
    starts = [sum(CHUNKS[:j]) for j in range(nch)]
    n_jobs = [0] + [n_loc // p for p in PACK[1:]]
    base = [sum(n_jobs[:j]) for j in range(nch + 1)]
    sd_base = 41 + base[nch]
    me = lax.axis_index("ep")

    def peer(k):
        return jnp.bitwise_xor(me, k)

    barrier = pltpu.get_barrier_semaphore()
    for k in range(1, n_dev):
        pl.semaphore_signal(barrier, inc=1, device_id={"ep": peer(k)}, device_id_type=MESH)

    def to_slot(src, slot, rows=None, cols=None):
        dst = ring.at[slot]
        if rows is not None:
            dst = ring.at[slot, pl.ds(0, rows), pl.ds(0, cols)]
        return pltpu.make_async_copy(src, dst, ring_sem.at[slot])

    wq_cols = []
    for i in range(3):
        for b, w in tiles(min(inter, w_q.shape[1] - i * inter), 768):
            wq_cols.append((i, b, w))

    def wq_job(p):
        i, b, w = wq_cols[p]
        return pltpu.make_async_copy(w_q.at[:, pl.ds(i * inter + b, w)], ring.at[i, :, pl.ds(b, w)], q_sem.at[p])

    def wo_job(i):
        a = i * inter
        w = min(inter, hid - a)
        return to_slot(w_o.at[:, pl.ds(a, w)], 3 + i, heads * vh, w)

    def sgu_job(i):
        src = s_gate if i % 2 == 0 else s_up
        return to_slot(src.at[:, pl.ds((i // 2) * inter, inter)], (5 + i) % NSLOT)

    def gate_job(e):
        return to_slot(e_gate.at[e], lax.rem(9 + 2 * e, NSLOT))

    def up_job(e):
        return to_slot(e_up.at[e], lax.rem(10 + 2 * e, NSLOT))

    def down_job(j, t):
        slot = lax.rem(41 + base[j] + t, NSLOT)
        return [pltpu.make_async_copy(e_down.at[t * PACK[j] + q, :, pl.ds(starts[j], CHUNKS[j])],
                                      ring.at[slot, pl.ds(0, inter), pl.ds(q * CHUNKS[j], CHUNKS[j])],
                                      ring_sem.at[slot] if PACK[j] == 1 else d_sem.at[slot, q]) for q in range(PACK[j])]

    def start_down(j, t):
        for c in down_job(j, t):
            c.start()

    def sd_job(i):
        r = i % 2
        c = i // 2
        half = hid // 2
        return to_slot(s_down.at[pl.ds(r * inter, inter), pl.ds(c * half, half)], (sd_base + i) % NSLOT, inter, half)

    def cache_job(g):
        s = lax.rem(g, NCACHE)
        n = GROUP * kvd
        return pltpu.make_async_copy(cache.at[pl.ds(pl.multiple_of(g * n, n), n)], cbuf.at[pl.ds(pl.multiple_of(s * n, n), n)], c_sem.at[s])

    def early_down(e):
        return pltpu.make_async_copy(e_down.at[e, :, pl.ds(0, CHUNKS[0])], cbuf.at[pl.ds(pl.multiple_of(e * inter, inter), inter)], e_sem.at[e])

    dkv_a = inter - 256
    dkv_copies = [pltpu.make_async_copy(w_dkv.at[:, pl.ds(0, dkv_a)], ring.at[2, pl.ds(0, kvd), pl.ds(256, dkv_a)], w_sem.at[0]),
                  pltpu.make_async_copy(w_dkv.at[:, pl.ds(dkv_a, hid - dkv_a)], ring.at[2, pl.ds(kvd, kvd), pl.ds(256, hid - dkv_a)], w_sem.at[3])]
    uk_copy = pltpu.make_async_copy(w_uk, uk_b, w_sem.at[1])
    uv_copy = pltpu.make_async_copy(w_uv, uv_b, w_sem.at[2])
    small = [pltpu.make_async_copy(a, b, in_sem.at[i]) for i, (a, b) in enumerate(
        ((x_h, x), (lens, lens_s), (lens_row, lens_v), (inv_h, inv), (ids_h, ids), (rw_h, rw)))]
    for c in small:
        c.start()
    for p in range(3):
        wq_job(p).start()
    for c in small:
        c.wait()

    col = iota((bsz, 128), 1)
    expert = iota((128, bsz), 0)
    gw = jnp.zeros((128, bsz), F32)
    for k in range(ids.shape[0]):
        gw = gw + jnp.where(ids[k:k + 1, :] == expert, rw[k:k + 1, :], 0.0)
    gw_all[pl.ds(pl.multiple_of(me * bsz, bsz), bsz), :] = gw.T

    diag = iota((bsz, bsz), 0) == iota((bsz, bsz), 1)
    pos = jnp.sum(jnp.where(diag, jnp.broadcast_to(lens_v[...], (bsz, bsz)), 0), axis=1, keepdims=True).astype(F32)
    ang = pos * inv[...]
    cs = jnp.cos(ang)
    half = (kvd - kvl) // 2
    low = col < half
    sn = jnp.where(low, -1.0, 1.0) * jnp.sin(ang)

    def rope(v):
        sw = jnp.where(low, pltpu.roll(v, 128 - half, 1), pltpu.roll(v, half, 1))
        return v * cs + sw * sn

    xf = x[...].astype(F32)
    xn = rms(xf).astype(BF16)

    pl.semaphore_wait(barrier, n_dev - 1)

    def gw_copy(k):
        mine = gw_all.at[pl.ds(pl.multiple_of(me * bsz, bsz), bsz)]
        return pltpu.make_async_remote_copy(mine, mine, gw_send.at[k - 1], gw_recv.at[k - 1], device_id={"ep": peer(k)}, device_id_type=MESH)

    for k in range(1, n_dev):
        gw_copy(k).start()

    following = [[wq_job(3)], [wq_job(4)] + dkv_copies, [uk_copy, cache_job(0)], [cache_job(1)], [cache_job(2)]]
    for p, (i, b, w) in enumerate(wq_cols):
        wq_job(p).wait()
        for c in following[p]:
            c.start()
        a = i * inter + b
        q_s[:, a:a + w] = dot(xn, ring[i, :, b:b + w]).astype(BF16)
    for c in dkv_copies:
        c.wait()
    kv = dot_nt(xn[:, :dkv_a], ring[2, :kvd, 256:]) + dot_nt(xn[:, dkv_a:], ring[2, kvd:2 * kvd, 256:256 + hid - dkv_a])
    kv_s[...] = jnp.zeros_like(kv_s)
    kv_s[:, :kvd] = kv
    kvn[:, :kvl] = rms(kv_s[:, :kvl]).astype(BF16)
    kvn[:, kvl:] = rope(kv_s[:, kvl:kvl + 128])[:, :kvd - kvl].astype(BF16)

    uk_copy.wait()
    cache_job(3).start()
    left = col < 64

    def put_head(h, q_nope, q_rot):
        ql = dot(q_nope.astype(BF16), uk_b[h])
        for c in range(nlat):
            qf[c, pl.ds(h, bsz, stride=heads), :] = ql[:, 128 * c:128 * (c + 1)]
        qf[nlat, pl.ds(h, bsz, stride=heads), :] = jnp.where(left, rope(q_rot), 0.0)

    for hp in range(heads // 2):
        a = hp * 2 * qkd
        b0 = q_s[:, a:a + 128].astype(F32)
        b1 = q_s[:, a + 128:a + 256].astype(F32)
        b2 = q_s[:, a + 256:a + 384].astype(F32)
        r1 = pltpu.roll(b1, 64, 1)
        r2 = pltpu.roll(b2, 64, 1)
        put_head(2 * hp, b0, b1)
        put_head(2 * hp + 1, jnp.where(left, r1, r2), r2)

    scale = qkd ** -0.5
    n_groups = bsz // GROUP
    tpos = iota((heads, lmax), 1)
    seq_of_row = iota((grows, bsz), 0) // heads
    seq_col = iota((grows, bsz), 1)

    def seq_rows(s, i, n):
        return pl.ds(pl.multiple_of((s * GROUP + i) * kvd, 64), n)

    def attend(g, carry):
        s = lax.rem(g, NCACHE)
        cache_job(g).wait()

        @pl.when(g + 4 < n_groups)
        def _():
            cache_job(g + 4).start()

        for k, group in enumerate(([uv_copy], [wo_job(1)], [wo_job(0)], [sgu_job(0)], [sgu_job(1)], [sgu_job(2)], [sgu_job(3)])):
            @pl.when(g == k)
            def _():
                for c in group:
                    c.start()
        rows = pl.ds(pl.multiple_of(g * grows, grows), grows)
        qg = jnp.concatenate([qf[c, rows, :].astype(BF16) for c in range(nlat + 1)], axis=1)[:, :kvd]
        own = seq_col == seq_of_row + g * GROUP
        s_new = jnp.sum(jnp.where(own, dot_nt(qg, kvn[...]), 0.0), axis=1, keepdims=True) * scale
        parts = []
        for i in range(GROUP):
            si = dot(qg[i * heads:(i + 1) * heads], cbuf[seq_rows(s, i, kvd), :]) * scale
            parts.append(jnp.where(tpos < lens_s[g * GROUP + i], si, -jnp.inf))
        sc = jnp.concatenate(parts, axis=0)
        mx = jnp.maximum(jnp.max(sc, axis=1, keepdims=True), s_new)
        e = jnp.exp(sc - mx)
        e_new = jnp.exp(s_new - mx)
        den = jnp.sum(e, axis=1, keepdims=True) + e_new
        rden = 1.0 / den
        p = (e * rden).astype(BF16)
        p_new = jnp.where(own, e_new * rden, 0.0).astype(BF16)
        o_new = dot(p_new, kvn[:, :kvl])
        outs_i = [dot_nt(p[i * heads:(i + 1) * heads], cbuf[seq_rows(s, i, kvl), :]) for i in range(GROUP)]
        o_lat = jnp.concatenate(outs_i, axis=0) + o_new
        for c in range(nlat):
            qf[c, rows, :] = o_lat[:, 128 * c:128 * (c + 1)]
        return carry

    lax.fori_loop(0, n_groups, attend, 0)
    uv_copy.wait()
    def o_lat_of(h):
        return jnp.concatenate([qf[c, pl.ds(h, bsz, stride=heads), :].astype(BF16) for c in range(nlat)], axis=1)

    for h in range(0, heads, 2):
        both = dot(jnp.concatenate([o_lat_of(h), o_lat_of(h + 1)], axis=0), jnp.concatenate([uv_b[h], uv_b[h + 1]], axis=1))
        o_s[:, h * vh:(h + 1) * vh] = both[:bsz, :vh].astype(BF16)
        o_s[:, (h + 1) * vh:(h + 2) * vh] = both[bsz:, vh:].astype(BF16)
    for i in range(2):
        wo_job(i).wait()
        a = i * inter
        for b, w in tiles(min(inter, hid - a), 512):
            h1_s[:, a + b:a + b + w] = (x[:, a + b:a + b + w].astype(F32) + dot(o_s[...], ring[3 + i, :, b:b + w])).astype(BF16)
    gate_job(0).start()
    up_job(0).start()

    def start_early(e, carry):
        early_down(e).start()
        return carry

    lax.fori_loop(0, n_loc, start_early, 0)

    u = rms(h1_s[...].astype(F32)).astype(BF16)
    mine = pl.ds(pl.multiple_of(me * bsz, bsz), bsz)
    across = pl.ds(pl.multiple_of(peer(2) * bsz, bsz), bsz)
    u_all[mine, :] = u

    def u_copy(rows, i, k):
        blk = u_all.at[rows]
        return pltpu.make_async_remote_copy(blk, blk, u_send.at[i], u_recv.at[i], device_id={"ep": peer(k)}, device_id_type=MESH)

    u_copy(mine, 1, 2).start()
    u_copy(mine, 0, 1).start()

    def shared_gu(i):
        for j in range(2):
            sgu_job(2 * i + j).wait()
        uu = u_all[mine, :]
        for b, w in tiles(inter, 512):
            gg = dot(uu, ring[(5 + 2 * i) % NSLOT, :, b:b + w])
            vv = dot(uu, ring[(6 + 2 * i) % NSLOT, :, b:b + w])
            acts_sh[:, i * inter + b:i * inter + b + w] = (silu(gg) * vv).astype(BF16)

    shared_gu(0)
    gate_job(1).start()
    up_job(1).start()
    shared_gu(1)
    gate_job(2).start()
    up_job(2).start()

    for k in range(1, n_dev):
        gw_copy(k).wait()
    nt = n_dev * bsz
    ga = gw_all[...]
    hit = ga > 0.0
    ti = iota((nt, nt), 0)
    tj = iota((nt, nt), 1)
    before = ((ti // bsz == tj // bsz) & (tj < ti)).astype(F32).astype(BF16)
    rank = dot(before, jnp.where(hit, 1.0, 0.0).astype(BF16))
    src = (iota((nt, 128), 0) // bsz * cape).astype(F32)
    code = jnp.where(hit, src + rank, -1.0)
    exp_r = iota((128, n_loc * rows_e), 0)
    exp_c = iota((128, n_loc * rows_e), 1) // rows_e
    spread = (exp_r == exp_c + me * n_loc).astype(F32).astype(BF16)
    code_x = dot(code.astype(BF16), spread)
    slot_c = (iota((nt, n_loc * rows_e), 1) % rows_e).astype(F32)
    member = code_x == slot_c
    g1 = ga.astype(BF16)
    res = ga - g1.astype(F32)
    g2 = res.astype(BF16)
    g3 = (res - g2.astype(F32)).astype(BF16)
    for t, gt in enumerate((g1, g2, g3)):
        w_s[t] = jnp.where(member, dot(gt, spread), 0.0).astype(BF16)
    d_s[...] = jnp.where(member, 1.0, 0.0).T.astype(BF16)

    u_copy(mine, 1, 2).wait_recv()
    u_copy(across, 2, 1).start()
    u_copy(mine, 0, 1).wait()
    u_copy(across, 2, 1).wait()
    u_copy(mine, 1, 2).wait_send()

    def gate_up(e, carry):
        erows = pl.ds(pl.multiple_of(e * rows_e, rows_e), rows_e)
        de = d_s[erows, :]
        for b, w in tiles(hid, 512):
            xr[:, b:b + w] = dot(de, u_all[:, b:b + w]).astype(BF16)
        gate_job(e).wait()
        up_job(e).wait()
        sg = lax.rem(9 + 2 * e, NSLOT)
        su = lax.rem(10 + 2 * e, NSLOT)
        for b, w in tiles(inter, 512):
            gg = dot(xr[...], ring[sg, :, b:b + w])
            vv = dot(xr[...], ring[su, :, b:b + w])
            acts[erows, b:b + w] = (silu(gg) * vv).astype(BF16)

        @pl.when(e + 3 < n_loc)
        def _():
            gate_job(e + 3).start()
            up_job(e + 3).start()

        @pl.when(e + 3 >= n_loc)
        def _():
            start_down(1, 2 * (e + 3 - n_loc))
            start_down(1, 2 * (e + 3 - n_loc) + 1)

        early_down(e).wait()
        outs[erows, :CHUNKS[0]] = dot(acts[erows, :], cbuf[pl.ds(pl.multiple_of(e * inter, inter), inter), :]).astype(BF16)
        return carry

    lax.fori_loop(0, n_loc, gate_up, 0)

    def part(j, d):
        return pl.ds(pl.multiple_of(PLACE[j][0] * nt + d * bsz, bsz), bsz)

    def blocks(j):
        return range(starts[j] // 128, (starts[j] + CHUNKS[j]) // 128)

    def pair_copy(j, i, d):
        return pltpu.make_async_remote_copy(qf.at[pl.ds(PLACE[j][1], len(blocks(j))), part(j, d)], rp.at[i, pl.ds(blocks(j)[0], len(blocks(j)))],
                                            p_send.at[j, i], p_recv.at[j, i], device_id={"ep": peer(1)}, device_id_type=MESH)

    def cross_copy(j):
        blk = pl.ds(blocks(j)[0], len(blocks(j)))
        return pltpu.make_async_remote_copy(xs.at[blk], rc.at[blk], x_send.at[j], x_recv.at[j],
                                            device_id={"ep": peer(2)}, device_id_type=MESH)

    def start_pair(j):
        pair_copy(j, 1, peer(3)).start()
        pair_copy(j, 0, peer(1)).start()

    def forward(j):
        pair_copy(j, 1, peer(3)).wait_recv()
        for c, b in enumerate(blocks(j)):
            xs[b] = qf[PLACE[j][1] + c, part(j, peer(2)), :] + rp[1, b]
        cross_copy(j).start()

    for j in range(nch):
        cw = CHUNKS[j]

        def down(t, carry):
            for c in down_job(j, t):
                c.wait()
            slot = lax.rem(41 + base[j] + t, NSLOT)
            for q in range(PACK[j]):
                erows = pl.ds(pl.multiple_of((t * PACK[j] + q) * rows_e, rows_e), rows_e)
                outs[erows, :cw] = dot(acts[erows, :], ring[slot, :inter, q * cw:(q + 1) * cw]).astype(BF16)
            for j2 in range(j, nch):
                first = base[j] + NSLOT - base[j2]
                if first + n_jobs[j] > 0 and first < n_jobs[j2]:
                    @pl.when((t + first >= 0) & (t + first < n_jobs[j2]))
                    def _():
                        start_down(j2, t + first)
            for k in range(4):
                if base[j] <= base[nch] + k - NSLOT < base[j + 1]:
                    @pl.when(t == base[nch] + k - NSLOT - base[j])
                    def _():
                        sd_job(k).start()
            if j >= 1:
                @pl.when(t == n_jobs[j] // 2)
                def _():
                    forward(j - 1)
            return carry

        if j > 0:
            lax.fori_loop(0, n_jobs[j], down, 0)
        ov = outs[:, :cw]
        total = dot(w_s[0], ov) + dot(w_s[1], ov) + dot(w_s[2], ov)
        for c in range(cw // 128):
            qf[PLACE[j][1] + c, pl.ds(PLACE[j][0] * nt, nt), :] = total[:, 128 * c:128 * (c + 1)]
        start_pair(j)
    forward(nch - 1)

    hw = hid // 2

    def finish(j):
        pair_copy(j, 0, peer(1)).wait_recv()
        cross_copy(j).wait_recv()
        for c, b in enumerate(blocks(j)):
            cols = slice(b * 128, (b + 1) * 128)
            routed = qf[PLACE[j][1] + c, part(j, me), :] + rp[0, b] + rc[b]
            y[:, cols] = (h1_s[:, cols].astype(F32) + sh[:, cols] + routed).astype(BF16)

    for k in range(4):
        c, r = k // 2, k % 2
        if k == 2:
            finish(0)
            finish(1)
        sd_job(k).wait()
        for b, w in tiles(hw, 512):
            cols = slice(c * hw + b, c * hw + b + w)
            acc = dot(acts_sh[:, r * inter:(r + 1) * inter], ring[(sd_base + k) % NSLOT, :inter, b:b + w])
            sh[:, cols] = acc if r == 0 else sh[:, cols] + acc
    for j in range(2, nch):
        finish(j)
    for j in range(nch):
        pair_copy(j, 1, peer(3)).wait_send()
        pair_copy(j, 0, peer(1)).wait_send()
        cross_copy(j).wait_send()


def solution(mesh):
    n = mesh.shape['ep']
    tok_spec = P(('rep', 'ep'))
    row_spec = P(('rep', 'ep'), None)
    cache_spec = P(('rep', 'ep'), None, None)
    exp_spec = P('ep', None, None)

    def local(x, cache, lens, ids, rw, w_q, w_dkv, w_uk, w_uv, w_o, s_gate, s_up, s_down, e_gate, e_up, e_down):
        bsz, hid = x.shape
        heads, nope, kvl = w_uk.shape
        lmax, kvd = cache.shape[1:]
        n_loc, _, inter = e_gate.shape
        top = ids.shape[1]
        n_exp = n_loc * n
        cape = (CAP_FACTOR * bsz * top + n_exp - 1) // n_exp
        rows_e = n * cape
        nt = n * bsz
        half = (kvd - kvl) // 2
        inv = np.float64(ROPE_BASE) ** (-2.0 * (np.arange(128) % half) / (kvd - kvl))
        inv = jnp.asarray(inv.astype(np.float32)[None, :])
        vm = pl.BlockSpec(memory_space=pltpu.VMEM)
        hb = pl.BlockSpec(memory_space=pl.ANY)
        dma = pltpu.SemaphoreType.DMA
        call = pl.pallas_call(
            lambda *refs: layer_kernel(cape, *refs),
            name="layer",
            out_shape=(pltpu.VMEM((bsz, hid), BF16), pltpu.VMEM((bsz, kvd), BF16)),
            in_specs=[hb] * 18,
            out_specs=(vm, vm),
            scratch_shapes=[
                pltpu.SMEM((bsz,), jnp.int32),
                pltpu.VMEM((1, bsz), jnp.int32),
                pltpu.VMEM((1, 128), F32),
                pltpu.VMEM((bsz, hid), BF16),
                pltpu.VMEM((top, bsz), jnp.int32),
                pltpu.VMEM((top, bsz), F32),
                pltpu.VMEM((NSLOT, hid, inter), BF16),
                pltpu.VMEM((NCACHE * GROUP * kvd, lmax), BF16),
                pltpu.VMEM(w_uk.shape, BF16),
                pltpu.VMEM(w_uv.shape, BF16),
                pltpu.VMEM((bsz, w_q.shape[1]), BF16),
                pltpu.VMEM((kvl // 128 + 1, bsz * heads, 128), F32),
                pltpu.VMEM((bsz, kvl + 128), F32),
                pltpu.VMEM((bsz, hid), BF16),
                pltpu.VMEM((bsz, hid), BF16),
                pltpu.VMEM((nt, hid), BF16),
                pltpu.VMEM((nt, 128), F32),
                pltpu.VMEM((n_loc * rows_e, nt), BF16),
                pltpu.VMEM((3, nt, n_loc * rows_e), BF16),
                pltpu.VMEM((rows_e, hid), BF16),
                pltpu.VMEM((n_loc * rows_e, inter), BF16),
                pltpu.VMEM((bsz, 2 * inter), BF16),
                pltpu.VMEM((n_loc * rows_e, max(CHUNKS)), BF16),
                pltpu.VMEM((2, hid // 128, bsz, 128), F32),
                pltpu.VMEM((hid // 128, bsz, 128), F32),
                pltpu.VMEM((hid // 128, bsz, 128), F32),
                pltpu.VMEM((bsz, hid), F32),
                dma((6,)), dma((5,)), dma((n_loc,)), dma((NSLOT,)), dma((NSLOT, max(PACK))), dma((NCACHE,)), dma((4,)),
                dma((n - 1,)), dma((n - 1,)), dma((3,)), dma((3,)),
                dma((len(CHUNKS), 2)), dma((len(CHUNKS), 2)), dma((len(CHUNKS),)), dma((len(CHUNKS),)),
            ],
            compiler_params=pltpu.CompilerParams(collective_id=0, has_side_effects=True, vmem_limit_bytes=66_600_000),
        )
        return call(lens, lens.reshape(1, bsz), inv, x, ids.T, rw.T, cache.transpose(0, 2, 1).reshape(bsz * kvd, lmax), w_q, w_dkv.T, w_uk, w_uv, w_o,
                    s_gate, s_up, s_down, e_gate, e_up, e_down)

    in_specs = (row_spec, cache_spec, tok_spec, row_spec, row_spec) + (P(),) * 8 + (exp_spec,) * 3
    return jax.shard_map(local, mesh=mesh, in_specs=in_specs, out_specs=(row_spec, row_spec), check_vma=False)
```
